32 devices in a mesh: rep: 16 (over z, y, core), grp: 2 (over x).
Axes of the slice: x: 2, y: 2, z: 4, core: 2. Of those that a mesh axis runs over, the one named last changes fastest.
Arguments:
- tokens: bfloat16 [24576, 768], P(('rep', 'grp')), may hold values from -6 to 6
- query_weight: bfloat16 [1536, 768], P('grp'), may hold values from -0.21875 to 0.21875
- key_weight: bfloat16 [256, 768], P('grp'), may hold values from -0.21875 to 0.21875
- value_weight: bfloat16 [256, 768], P('grp'), may hold values from -0.21875 to 0.21875
- query_bias: bfloat16 [1536], P('grp'), may hold values from -3 to 3
- key_bias: bfloat16 [256], P('grp'), may hold values from -3 to 3
- value_bias: bfloat16 [256], P('grp'), may hold values from -3 to 3
- output_matrix: bfloat16 [768, 1536], P('grp'), may hold values from -0.625 to 0.625
- gate_weight: bfloat16 [4480, 768], P('grp'), may hold values from -0.21875 to 0.21875
- up_weight: bfloat16 [4480, 768], P('grp'), may hold values from -0.21875 to 0.21875
- down_weight: bfloat16 [768, 4480], P('grp'), may hold values from -0.09375 to 0.09375
- attn_gain: bfloat16 [768], P('grp'), may hold values from 0.5 to 1.5
- mlp_gain: bfloat16 [768], P('grp'), may hold values from 0.5 to 1.5
- cotangent: bfloat16 [24576, 768], P(('rep', 'grp')), may hold values from -6 to 6
- seq_lengths: int32 [32, 4], P(('rep', 'grp')), may hold values from 1 to 512, 768 in all within a row
Outputs:
- block_out: float32 [24576, 768], P(('rep', 'grp'))
- input_grad: float32 [24576, 768], P(('rep', 'grp'))
- query_weight_grad: float32 [1536, 768], P('grp')
- key_weight_grad: float32 [256, 768], P('grp')
- value_weight_grad: float32 [256, 768], P('grp')
- query_bias_grad: float32 [1536], P('grp')
- key_bias_grad: float32 [256], P('grp')
- value_bias_grad: float32 [256], P('grp')
- output_weight_grad: float32 [768, 1536], P('grp')
- gate_weight_grad: float32 [4480, 768], P('grp')
- up_weight_grad: float32 [4480, 768], P('grp')
- down_weight_grad: float32 [768, 4480], P('grp')
- attn_gain_grad: float32 [768], P('grp')
- mlp_gain_grad: float32 [768], P('grp')
The draws below stay inside these ranges and needn't reach their ends.
Inputs may be any that keep to these rules, and one draw needn't show every extreme that they name: `seq_lengths`: each row lists the lengths of the 4 sequences packed on one device; each row sums to 768 and its largest entry is exactly 512.
All inputs are finite; a program needn't handle non-finite values.
Results may differ from the reference program's by a relative error of at most 0.023.
Values may be sent and summed in bfloat16 or wider, within the bound.
A program may use at most 320 MiB of HBM per device.

```python
import math
import jax
import jax.numpy as jnp
import numpy as np
from jax import lax

D = 768
FF = 4480
QUERY_HEADS = 12
KEY_VALUE_HEADS = 2
HEAD_SIZE = 128
TOK_DEV = 768
SEQ_DEV = 4
SEQ_MAX = 512
QW = 1536
KW = 256
TOKENS = 24576
N_REP = 16
N_GRP = 2


def block_scale(key, dims, pieces, smallest, high):
    def one(axis_at, shards_of):
        heights = jax.random.uniform(jax.random.fold_in(jax.random.fold_in(key, 6), axis_at), (shards_of,), jnp.float32, smallest / len(pieces), high / len(pieces))
        return jnp.repeat(jnp.exp(heights), dims[axis_at] // shards_of).reshape((-1,) + (1,) * (len(dims) - axis_at - 1))

    factor_of = one(*pieces[0])
    for cut in pieces[1:]:
        factor_of = factor_of * one(*cut)
    return factor_of


def length_profile(amount, total, limit, skew):
    loads = [(1 << 20) // math.isqrt(standing ** skew) + 1 for standing in range(2, amount + 1)]
    surplus, counts = total - limit - (amount - 1), [1] * (amount - 1)
    while surplus > 0:
        free = [i for i in range(amount - 1) if counts[i] < limit]
        whole, budget = sum([loads[i] for i in free]), surplus
        for i in free:
            more = min(limit - counts[i], max(1, budget * loads[i] // whole), surplus)
            counts[i] = counts[i] + more
            surplus = surplus - more
    return np.array([limit] + counts)


def ragged(rng, number_of, total, limit, lean):
    if number_of == 2:
        one = jax.random.randint(rng, (), max(1, total - limit), min(limit, total - 1) + 1)
        return jnp.stack([one, total - one])
    lengths = jnp.asarray(length_profile(number_of, total, limit, lean), jnp.int32)
    pairs = (number_of - 1) // 2
    giver, sink = lengths[1:1 + 2 * pairs:2], lengths[2:2 + 2 * pairs:2]
    margin = jnp.minimum(giver - 1, limit - sink)
    moved = jax.random.randint(jax.random.fold_in(rng, 1), (pairs,), 0, 1 << 20) % (margin + 1)
    lengths = lengths.at[1:1 + 2 * pairs:2].set(giver - moved).at[2:2 + 2 * pairs:2].set(sink + moved)
    return lengths[jax.random.permutation(jax.random.fold_in(rng, 2), number_of)]


def scatter_about(rng, shape, deviation, most, split=(), kind=jnp.bfloat16):
    factor_of = block_scale(rng, shape, split, -0.22, 0.18) if split else 1.0
    drawn = jax.random.normal(rng, shape, jnp.float32) * deviation * factor_of
    return jnp.minimum(jnp.maximum(drawn, -most), most).astype(kind)


def setup_inputs(seed: int = 0) -> dict:
    arg_keys = jax.random.split(jax.random.key(seed), 16)
    return {
        "tokens": scatter_about(arg_keys[0], (TOKENS, D), 1.0, 6.0, ((0, 32),)),
        "query_weight": scatter_about(arg_keys[1], (QW, D), D ** -0.5, 0.21875, ((0, 2),)),
        "key_weight": scatter_about(arg_keys[2], (KW, D), D ** -0.5, 0.21875, ((0, 2),)),
        "value_weight": scatter_about(arg_keys[3], (KW, D), D ** -0.5, 0.21875, ((0, 2),)),
        "query_bias": scatter_about(arg_keys[4], (QW,), 0.5, 3.0, ((0, 2),)),
        "key_bias": scatter_about(arg_keys[5], (KW,), 0.5, 3.0, ((0, 2),)),
        "value_bias": scatter_about(arg_keys[6], (KW,), 0.5, 3.0, ((0, 2),)),
        "output_matrix": scatter_about(arg_keys[7], (D, QW), (QW // 16) ** -0.5, 0.625, ((0, 2),)),
        "gate_weight": scatter_about(arg_keys[8], (FF, D), D ** -0.5, 0.21875, ((0, 2),)),
        "up_weight": scatter_about(arg_keys[9], (FF, D), D ** -0.5, 0.21875, ((0, 2),)),
        "down_weight": scatter_about(arg_keys[10], (D, FF), FF ** -0.5, 0.09375, ((0, 2),)),
        "attn_gain": jnp.clip(1.0 + 0.1 * jax.random.normal(arg_keys[11], (D,), jnp.float32), 0.5, 1.5).astype(jnp.bfloat16),
        "mlp_gain": jnp.clip(1.0 + 0.1 * jax.random.normal(arg_keys[12], (D,), jnp.float32), 0.5, 1.5).astype(jnp.bfloat16),
        "cotangent": scatter_about(arg_keys[13], (TOKENS, D), 1.0, 6.0, ((0, 32),)),
        "seq_lengths": jax.vmap(lambda own: ragged(own, SEQ_DEV, TOK_DEV, SEQ_MAX, 2))(jax.random.split(arg_keys[14], (N_REP * N_GRP))).reshape((N_REP * N_GRP, SEQ_DEV)).astype(jnp.int32),
    }


EPSILON = 1e-06
THETA = 1000000.0

def contract(form, left, right):
    return jnp.einsum(form, left.astype(jnp.float32), right.astype(jnp.float32))

def layout(seq_lengths, count_of_rows):
    lengths_int = seq_lengths.astype(jnp.int32)
    seq_ends = jnp.cumsum(lengths_int).astype(jnp.int32)
    seq_starts = (seq_ends - lengths_int).astype(jnp.int32)
    row_index = jnp.arange(count_of_rows, dtype=jnp.int32)
    segment = lax.optimization_barrier(jnp.sum((row_index[:, None] >= seq_ends[None, :]).astype(jnp.int32), axis=1)).astype(jnp.int32)
    member = segment[:, None] == jnp.arange(lengths_int.shape[0], dtype=jnp.int32)[None, :]
    position = (row_index - lax.optimization_barrier(jnp.sum(jnp.where(member, seq_starts[None, :], 0), axis=1))).astype(jnp.int32)
    allowed = (segment[:, None] == segment[None, :]) & (row_index[None, :] <= row_index[:, None])
    return (position, allowed)

def rotary_tables(position, head_dim):
    half_dim = head_dim // 2
    exponent = jnp.arange(half_dim, dtype=jnp.float32) * (2.0 / head_dim)
    frequency = jnp.exp(-exponent * math.log(THETA))
    angles = position.astype(jnp.float32)[:, None] * frequency[None, :]
    cosine_lookup = jnp.concatenate([jnp.cos(angles), jnp.cos(angles)], axis=-1)
    sine_lookup = jnp.concatenate([jnp.sin(angles), jnp.sin(angles)], axis=-1)
    return (cosine_lookup, sine_lookup)

def apply_rotary(vectors, cosine_lookup, sine_lookup):
    half_dim = vectors.shape[-1] // 2
    turned = jnp.concatenate([-vectors[..., half_dim:], vectors[..., :half_dim]], axis=-1)
    return vectors * cosine_lookup[:, None, :] + turned * sine_lookup[:, None, :]

def inverse_rotary(grads, cosine_lookup, sine_lookup):
    half_dim = grads.shape[-1] // 2
    scaled = grads * sine_lookup[:, None, :]
    turned = jnp.concatenate([scaled[..., half_dim:], -scaled[..., :half_dim]], axis=-1)
    return grads * cosine_lookup[:, None, :] + turned

def rms_scale(values):
    return lax.rsqrt(lax.optimization_barrier(jnp.mean(values * values, axis=-1, keepdims=True)) + EPSILON)

def attn_scores(query_rotated, key_rotated, allowed):
    scores = contract('tkgd,skd->kgts', query_rotated, key_rotated) * (1.0 / math.sqrt(HEAD_SIZE))
    return jnp.where(allowed, scores, -1e+30)

def forward_pass(tokens, seq_lengths, params):
    query_weight, key_weight, value_weight, query_bias, key_bias, value_bias, output_matrix, gate_weight, up_weight, down_weight, attn_gain, mlp_gain = params
    query_bias = query_bias.astype(jnp.float32)
    key_bias = key_bias.astype(jnp.float32)
    value_bias = value_bias.astype(jnp.float32)
    attn_gain = attn_gain.astype(jnp.float32)
    mlp_gain = mlp_gain.astype(jnp.float32)
    count_of_rows = tokens.shape[0]
    group_extent = QUERY_HEADS // KEY_VALUE_HEADS
    position, allowed = layout(seq_lengths, count_of_rows)
    cosine_lookup, sine_lookup = rotary_tables(position, HEAD_SIZE)
    inputs = tokens.astype(jnp.float32)
    scale_one = rms_scale(inputs)
    normed_one = (inputs * scale_one * attn_gain).astype(jnp.bfloat16)
    query_rows = jnp.dot(normed_one, query_weight.T, preferred_element_type=jnp.float32) + query_bias
    key_unrotated = jnp.dot(normed_one, key_weight.T, preferred_element_type=jnp.float32) + key_bias
    value_unexpanded = jnp.dot(normed_one, value_weight.T, preferred_element_type=jnp.float32) + value_bias
    query_rotated = apply_rotary(query_rows.reshape(count_of_rows, QUERY_HEADS, HEAD_SIZE), cosine_lookup, sine_lookup).astype(jnp.bfloat16).reshape(count_of_rows, KEY_VALUE_HEADS, group_extent, HEAD_SIZE)
    key_rotated = apply_rotary(key_unrotated.reshape(count_of_rows, KEY_VALUE_HEADS, HEAD_SIZE), cosine_lookup, sine_lookup).astype(jnp.bfloat16)
    value_blocks = value_unexpanded.reshape(count_of_rows, KEY_VALUE_HEADS, HEAD_SIZE).astype(jnp.bfloat16)
    scores = attn_scores(query_rotated, key_rotated, allowed)
    row_peak = lax.optimization_barrier(jnp.max(scores, axis=-1, keepdims=True))
    log_total = row_peak + jnp.log(lax.optimization_barrier(jnp.sum(jnp.exp(scores - row_peak), axis=-1, keepdims=True)))
    attn_probs = jnp.exp(scores - log_total).astype(jnp.bfloat16)
    attention_combined = contract('kgts,skd->tkgd', attn_probs, value_blocks).reshape(count_of_rows, QUERY_HEADS * HEAD_SIZE).astype(jnp.bfloat16)
    residual = inputs + jnp.dot(attention_combined, output_matrix.T, preferred_element_type=jnp.float32)
    scale_two = rms_scale(residual)
    normed_two = (residual * scale_two * mlp_gain).astype(jnp.bfloat16)
    gate_pre = jnp.dot(normed_two, gate_weight.T, preferred_element_type=jnp.float32)
    up_proj = jnp.dot(normed_two, up_weight.T, preferred_element_type=jnp.float32)
    hidden = (jax.nn.silu(gate_pre) * up_proj).astype(jnp.bfloat16)
    block_out = residual + jnp.dot(hidden, down_weight.T, preferred_element_type=jnp.float32)
    kept_state = (allowed, cosine_lookup, sine_lookup, inputs, scale_one, normed_one, query_rotated, key_rotated, value_blocks, log_total, attention_combined, residual, scale_two, normed_two, gate_pre, up_proj, hidden)
    return (block_out, kept_state)

def mlp_backward(kept_state, cotangent, down_weight, gate_weight, up_weight, mlp_gain):
    mlp_gain = mlp_gain.astype(jnp.float32)
    residual, scale_two, normed_two, gate_pre, up_proj, hidden = kept_state[11:]
    down_weight_grad = jnp.dot(cotangent.T, hidden, preferred_element_type=jnp.float32)
    hidden_grad = jnp.dot(cotangent, down_weight, preferred_element_type=jnp.float32)
    sigmoid_gate = jax.nn.sigmoid(gate_pre)
    activated = gate_pre * sigmoid_gate
    gate_grad = (hidden_grad * up_proj * sigmoid_gate * (1.0 + gate_pre * (1.0 - sigmoid_gate))).astype(jnp.bfloat16)
    up_grad = (hidden_grad * activated).astype(jnp.bfloat16)
    gate_weight_grad = jnp.dot(gate_grad.T, normed_two, preferred_element_type=jnp.float32)
    up_weight_grad = jnp.dot(up_grad.T, normed_two, preferred_element_type=jnp.float32)
    normed_grad = jnp.dot(gate_grad, gate_weight, preferred_element_type=jnp.float32) + jnp.dot(up_grad, up_weight, preferred_element_type=jnp.float32)
    unit_two = residual * scale_two
    mlp_gain_grad = lax.optimization_barrier(jnp.sum(normed_grad * unit_two, axis=0))
    unit_grad = normed_grad * mlp_gain
    residual_grad = cotangent.astype(jnp.float32) + scale_two * (unit_grad - unit_two * lax.optimization_barrier(jnp.mean(unit_grad * unit_two, axis=-1, keepdims=True)))
    return (residual_grad, (gate_weight_grad, up_weight_grad, down_weight_grad, mlp_gain_grad))

def attn_backward(kept_state, residual_grad, query_weight, key_weight, value_weight, output_matrix, attn_gain):
    attn_gain = attn_gain.astype(jnp.float32)
    allowed, cosine_lookup, sine_lookup, inputs, scale_one, normed_one, query_rotated, key_rotated, value_blocks, log_total, attention_combined = kept_state[:11]
    count_of_rows = residual_grad.shape[0]
    group_extent = QUERY_HEADS // KEY_VALUE_HEADS
    score_scale = 1.0 / math.sqrt(HEAD_SIZE)
    residual_gradient_blocks = residual_grad.astype(jnp.bfloat16)
    output_weight_grad = jnp.dot(residual_gradient_blocks.T, attention_combined, preferred_element_type=jnp.float32)
    combined_gradient = jnp.dot(residual_gradient_blocks, output_matrix, preferred_element_type=jnp.float32).astype(jnp.bfloat16).reshape(count_of_rows, KEY_VALUE_HEADS, group_extent, HEAD_SIZE)
    scores = attn_scores(query_rotated, key_rotated, allowed)
    attn_probs = jnp.exp(scores - log_total)
    probs_b = attn_probs.astype(jnp.bfloat16)
    value_gradient = contract('kgts,tkgd->skd', probs_b, combined_gradient)
    probs_grad = contract('tkgd,skd->kgts', combined_gradient, value_blocks)
    row_difference = lax.optimization_barrier(jnp.sum(combined_gradient.astype(jnp.float32) * attention_combined.reshape(count_of_rows, KEY_VALUE_HEADS, group_extent, HEAD_SIZE).astype(jnp.float32), axis=-1))
    row_difference = jnp.transpose(row_difference, (1, 2, 0))[..., None]
    score_grad = (attn_probs * (probs_grad - row_difference) * score_scale).astype(jnp.bfloat16)
    queries_grad = contract('kgts,skd->tkgd', score_grad, key_rotated).reshape(count_of_rows, QUERY_HEADS, HEAD_SIZE)
    key_gradient = contract('kgts,tkgd->skd', score_grad, query_rotated)
    queries_pre_grad = inverse_rotary(queries_grad, cosine_lookup, sine_lookup).reshape(count_of_rows, QUERY_HEADS * HEAD_SIZE)
    key_unrotated_gradient = inverse_rotary(key_gradient, cosine_lookup, sine_lookup).reshape(count_of_rows, KEY_VALUE_HEADS * HEAD_SIZE)
    value_unexpanded_gradient = value_gradient.reshape(count_of_rows, KEY_VALUE_HEADS * HEAD_SIZE)
    query_bias_grad = lax.optimization_barrier(jnp.sum(queries_pre_grad, axis=0))
    key_bias_grad = lax.optimization_barrier(jnp.sum(key_unrotated_gradient, axis=0))
    value_bias_grad = lax.optimization_barrier(jnp.sum(value_unexpanded_gradient, axis=0))
    queries_b = queries_pre_grad.astype(jnp.bfloat16)
    keys_b = key_unrotated_gradient.astype(jnp.bfloat16)
    values_gb = value_unexpanded_gradient.astype(jnp.bfloat16)
    query_weight_grad = jnp.dot(queries_b.T, normed_one, preferred_element_type=jnp.float32)
    key_weight_grad = jnp.dot(keys_b.T, normed_one, preferred_element_type=jnp.float32)
    value_weight_grad = jnp.dot(values_gb.T, normed_one, preferred_element_type=jnp.float32)
    normed_grad = jnp.dot(queries_b, query_weight, preferred_element_type=jnp.float32)
    normed_grad = normed_grad + jnp.dot(keys_b, key_weight, preferred_element_type=jnp.float32)
    normed_grad = normed_grad + jnp.dot(values_gb, value_weight, preferred_element_type=jnp.float32)
    unit_one = inputs * scale_one
    attn_gain_grad = lax.optimization_barrier(jnp.sum(normed_grad * unit_one, axis=0))
    unit_grad = normed_grad * attn_gain
    input_grad = residual_grad + scale_one * (unit_grad - unit_one * lax.optimization_barrier(jnp.mean(unit_grad * unit_one, axis=-1, keepdims=True)))
    return (input_grad, (query_weight_grad, key_weight_grad, value_weight_grad, query_bias_grad, key_bias_grad, value_bias_grad, output_weight_grad, attn_gain_grad))

def reference(tokens, query_weight, key_weight, value_weight, query_bias, key_bias, value_bias, output_matrix, gate_weight, up_weight, down_weight, attn_gain, mlp_gain, cotangent, seq_lengths):
    device_count = N_REP * N_GRP
    params = (query_weight, key_weight, value_weight, query_bias, key_bias, value_bias, output_matrix, gate_weight, up_weight, down_weight, attn_gain, mlp_gain)
    token_blocks = tokens.reshape(device_count, TOK_DEV, D)
    cot_blocks = cotangent.reshape(device_count, TOK_DEV, D)
    initial = tuple((jnp.zeros(shape_like.shape, jnp.float32) for shape_like in (query_weight, key_weight, value_weight, query_bias, key_bias, value_bias, output_matrix, attn_gain, gate_weight, up_weight, down_weight, mlp_gain)))

    def device_step(grad_sums, block_rows):
        token_rows, cot_rows, length_row = block_rows
        block_out, kept_state = forward_pass(token_rows, length_row, params)
        residual_grad, mlp_grads = mlp_backward(kept_state, cot_rows, down_weight, gate_weight, up_weight, mlp_gain)
        input_grad, attn_grads = attn_backward(kept_state, residual_grad, query_weight, key_weight, value_weight, output_matrix, attn_gain)
        grad_sums = jax.tree.map(jnp.add, grad_sums, attn_grads + mlp_grads)
        return (grad_sums, (block_out, input_grad))
    grad_sums, (outputs, input_grads) = lax.scan(device_step, initial, (token_blocks, cot_blocks, seq_lengths))
    return (outputs.reshape(TOKENS, D), input_grads.reshape(TOKENS, D), grad_sums[0], grad_sums[1], grad_sums[2], grad_sums[3], grad_sums[4], grad_sums[5], grad_sums[6], grad_sums[8], grad_sums[9], grad_sums[10], grad_sums[7], grad_sums[11])
```

```python
import math

import jax
import jax.numpy as jnp
from jax import lax
from jax.sharding import PartitionSpec as P

QUERY_HEADS = 12
KEY_VALUE_HEADS = 2
HEAD_SIZE = 128

EPSILON = 1e-06
THETA = 1000000.0

BF16 = jnp.bfloat16
F32 = jnp.float32


def contract(form, left, right):
    return jnp.einsum(form, left, right, preferred_element_type=F32)


def mm_nt(left, right):
    return lax.dot_general(left, right, (((1,), (1,)), ((), ())), preferred_element_type=F32)


def mm_nn(left, right):
    return lax.dot_general(left, right, (((1,), (0,)), ((), ())), preferred_element_type=F32)


def mm_tn(left, right):
    return lax.dot_general(left, right, (((0,), (0,)), ((), ())), preferred_element_type=F32)


def layout(seq_lengths, count_of_rows):
    seq_ends = jnp.cumsum(seq_lengths)
    seq_starts = seq_ends - seq_lengths
    row_index = jnp.arange(count_of_rows, dtype=jnp.int32)
    segment = jnp.sum((row_index[:, None] >= seq_ends[None, :]).astype(jnp.int32), axis=1)
    member = segment[:, None] == jnp.arange(seq_lengths.shape[0], dtype=jnp.int32)[None, :]
    position = row_index - jnp.sum(jnp.where(member, seq_starts[None, :], 0), axis=1)
    allowed = (segment[:, None] == segment[None, :]) & (row_index[None, :] <= row_index[:, None])
    return (position, allowed)


def rotary_tables(position, head_dim):
    half_dim = head_dim // 2
    exponent = jnp.arange(half_dim, dtype=F32) * (2.0 / head_dim)
    frequency = jnp.exp(-exponent * math.log(THETA))
    angles = position.astype(F32)[:, None] * frequency[None, :]
    cosine = jnp.cos(angles)
    sine = jnp.sin(angles)
    return (jnp.concatenate([cosine, cosine], axis=-1), jnp.concatenate([sine, sine], axis=-1))


def apply_rotary(vectors, cosine, sine):
    half_dim = vectors.shape[-1] // 2
    turned = jnp.concatenate([-vectors[..., half_dim:], vectors[..., :half_dim]], axis=-1)
    return vectors * cosine[:, None, :] + turned * sine[:, None, :]


def inverse_rotary(grads, cosine, sine):
    half_dim = grads.shape[-1] // 2
    scaled = grads * sine[:, None, :]
    turned = jnp.concatenate([scaled[..., half_dim:], -scaled[..., :half_dim]], axis=-1)
    return grads * cosine[:, None, :] + turned


def rms_scale(values):
    return lax.rsqrt(jnp.mean(values * values, axis=-1, keepdims=True) + EPSILON)


def swap(x):
    return lax.ppermute(x, "grp", [(0, 1), (1, 0)])


def in_order(mine, other, g, axis=0):
    first = jnp.where(g == 0, mine, other)
    second = jnp.where(g == 0, other, mine)
    return jnp.concatenate([first, second], axis)


def half_of(x, which, axis):
    size = x.shape[axis] // 2
    return lax.dynamic_slice_in_dim(x, which * size, size, axis)


def hop(x, bit, n):
    return lax.ppermute(x, "rep", [(i, i ^ (1 << bit)) for i in range(n)])


def sum_over_rep(x, order, me, n):
    for b in order:
        bit = (me >> b) & 1
        came = hop(half_of(x, 1 - bit, 0), b, n)
        x = (half_of(x, bit, 0).astype(F32) + came.astype(F32)).astype(BF16)
    for i, b in enumerate(reversed(order)):
        bit = (me >> b) & 1
        came = hop(x, b, n)
        if i == len(order) - 1:
            x, came = x.astype(F32), came.astype(F32)
        x = in_order(x, came, bit)
    return x


def attention_forward(query_rotated, key_rotated, values, allowed):
    scores = contract("thd,sd->hts", query_rotated, key_rotated) * (1.0 / math.sqrt(HEAD_SIZE))
    scores = jnp.where(allowed, scores, -1e30)
    row_peak = jnp.max(scores, axis=-1, keepdims=True)
    log_total = row_peak + jnp.log(jnp.sum(jnp.exp(scores - row_peak), axis=-1, keepdims=True))
    probs = jnp.exp(scores - log_total).astype(BF16)
    mixed = contract("hts,sd->thd", probs, values)
    return mixed.reshape(mixed.shape[0], -1).astype(BF16), log_total


def attention_backward(query_rotated, key_rotated, values, allowed, log_total, mixed, mixed_grad):
    heads = query_rotated.shape[1]
    rows = query_rotated.shape[0]
    score_scale = 1.0 / math.sqrt(HEAD_SIZE)
    mixed = mixed.reshape(rows, heads, HEAD_SIZE)
    mixed_grad = mixed_grad.reshape(rows, heads, HEAD_SIZE)
    scores = contract("thd,sd->hts", query_rotated, key_rotated) * score_scale
    scores = jnp.where(allowed, scores, -1e30)
    probs = jnp.exp(scores - log_total)
    values_grad = contract("hts,thd->sd", probs.astype(BF16), mixed_grad)
    probs_grad = contract("thd,sd->hts", mixed_grad, values)
    delta = jnp.sum(mixed_grad.astype(F32) * mixed.astype(F32), axis=-1)
    delta = jnp.transpose(delta, (1, 0))[..., None]
    score_grad = (probs * (probs_grad - delta) * score_scale).astype(BF16)
    queries_grad = contract("hts,sd->thd", score_grad, key_rotated)
    keys_grad = contract("hts,thd->sd", score_grad, query_rotated)
    return queries_grad, keys_grad, values_grad


def local(
    n_rep,
    tokens,
    query_weight,
    key_weight,
    value_weight,
    query_bias,
    key_bias,
    value_bias,
    output_matrix,
    gate_weight,
    up_weight,
    down_weight,
    attn_gain,
    mlp_gain,
    cotangent,
    seq_lengths,
):
    g = lax.axis_index("grp")
    me = lax.axis_index("rep")
    bits = n_rep.bit_length() - 1
    straight = tuple(range(bits))
    crossed = (0, 2, 1) + tuple(range(3, bits)) if bits >= 3 else straight
    rows = tokens.shape[0]
    heads = query_weight.shape[0] // HEAD_SIZE

    gains = jnp.stack([attn_gain, mlp_gain])
    gains_other = swap(gains)
    tokens_other = swap(tokens)
    lengths_other = swap(seq_lengths)
    output_other = swap(half_of(output_matrix, 1 - g, 1))
    down_other = swap(half_of(down_weight, 1 - g, 1))
    cotangent_other = swap(cotangent)
    gains = in_order(gains, gains_other, g, 1).astype(F32)
    attn_gain_all, mlp_gain_all = gains[0:1], gains[1:2]
    output_cols = in_order(half_of(output_matrix, g, 1), output_other, g)
    down_cols = in_order(half_of(down_weight, g, 1), down_other, g)

    def front(token_rows, lengths):
        position, allowed = layout(lengths[0], rows)
        cosine, sine = rotary_tables(position, HEAD_SIZE)
        inputs = token_rows.astype(F32)
        scale = rms_scale(inputs)
        normed = (inputs * scale * attn_gain_all).astype(BF16)
        queries = mm_nt(normed, query_weight) + query_bias.astype(F32)
        keys = mm_nt(normed, key_weight) + key_bias.astype(F32)
        values = (mm_nt(normed, value_weight) + value_bias.astype(F32)).astype(BF16)
        queries = apply_rotary(queries.reshape(rows, heads, HEAD_SIZE), cosine, sine).astype(BF16)
        keys = apply_rotary(keys[:, None, :], cosine, sine)[:, 0].astype(BF16)
        mixed, log_total = attention_forward(queries, keys, values, allowed)
        part = mm_nt(mixed, output_cols)
        return dict(
            inputs=inputs,
            scale=scale,
            normed=normed,
            queries=queries,
            keys=keys,
            values=values,
            mixed=mixed,
            log_total=log_total,
            part=part,
            allowed=allowed,
            cosine=cosine,
            sine=sine,
        )

    own = front(tokens, seq_lengths)
    came_other = swap(own["part"].astype(BF16))
    oth = front(tokens_other, lengths_other)
    came_own = swap(oth["part"].astype(BF16))
    residual_own = own["inputs"] + own["part"] + came_own.astype(F32)
    residual_oth = oth["inputs"] + oth["part"] + came_other.astype(F32)
    residual = jnp.concatenate([residual_own, residual_oth])
    cot = jnp.concatenate([cotangent, cotangent_other])

    scale_two = rms_scale(residual)
    normed_two = (residual * scale_two * mlp_gain_all).astype(BF16)
    gate_pre = mm_nt(normed_two, gate_weight)
    up_proj = mm_nt(normed_two, up_weight)
    hidden_grad = mm_nn(cot, down_cols)
    sigmoid = jax.nn.sigmoid(gate_pre)
    activated = gate_pre * sigmoid
    hidden = (activated * up_proj).astype(BF16)
    gate_grad = (hidden_grad * up_proj * sigmoid * (1.0 + gate_pre * (1.0 - sigmoid))).astype(BF16)
    up_grad = (hidden_grad * activated).astype(BF16)

    down_part = mm_nt(hidden, down_cols)
    down_came = swap(down_part[rows:].astype(BF16))
    block_out = residual_own + down_part[:rows] + down_came.astype(F32)

    down_grad = mm_tn(cot, hidden).astype(BF16)
    down_grad_came = swap(half_of(down_grad, 1 - g, 0))
    down_grad = in_order(half_of(down_grad, g, 0), down_grad_came, g, 1)
    down_weight_grad = sum_over_rep(down_grad, crossed, me, n_rep)
    gate_weight_grad = sum_over_rep(mm_tn(gate_grad, normed_two).astype(BF16), straight, me, n_rep)
    up_weight_grad = sum_over_rep(mm_tn(up_grad, normed_two).astype(BF16), straight, me, n_rep)

    normed_grad = mm_nn(gate_grad, gate_weight) + mm_nn(up_grad, up_weight)
    normed_came = swap(normed_grad.astype(BF16))
    normed_grad = normed_grad + jnp.concatenate([normed_came[rows:], normed_came[:rows]]).astype(F32)
    unit_two = residual * scale_two
    mlp_gain_grad = jnp.sum(normed_grad * unit_two, axis=0)
    unit_grad = normed_grad * mlp_gain_all
    residual_grad = cot.astype(F32) + scale_two * (
        unit_grad - unit_two * jnp.mean(unit_grad * unit_two, axis=-1, keepdims=True)
    )

    residual_grad_b = residual_grad.astype(BF16)
    mixed_both = jnp.concatenate([own["mixed"], oth["mixed"]])
    output_grad = mm_tn(residual_grad_b, mixed_both).astype(BF16)
    output_grad_came = swap(half_of(output_grad, 1 - g, 0))
    output_grad = in_order(half_of(output_grad, g, 0), output_grad_came, g, 1)
    output_weight_grad = sum_over_rep(output_grad, straight, me, n_rep)
    mixed_grad = mm_nn(residual_grad_b, output_cols).astype(BF16)

    def back(kept, mixed_grad):
        queries_grad, keys_grad, values_grad = attention_backward(
            kept["queries"],
            kept["keys"],
            kept["values"],
            kept["allowed"],
            kept["log_total"],
            kept["mixed"],
            mixed_grad,
        )
        queries_grad = inverse_rotary(queries_grad, kept["cosine"], kept["sine"]).reshape(rows, -1)
        keys_grad = inverse_rotary(keys_grad[:, None, :], kept["cosine"], kept["sine"])[:, 0]
        sums = (jnp.sum(queries_grad, 0), jnp.sum(keys_grad, 0), jnp.sum(values_grad, 0))
        return sums, (queries_grad.astype(BF16), keys_grad.astype(BF16), values_grad.astype(BF16))

    def front_grad(grads):
        queries_b, keys_b, values_b = grads
        return mm_nn(queries_b, query_weight) + mm_nn(keys_b, key_weight) + mm_nn(values_b, value_weight)

    sums_oth, grads_oth = back(oth, mixed_grad[rows:])
    grad_came = swap(front_grad(grads_oth).astype(BF16))
    sums_own, grads_own = back(own, mixed_grad[:rows])
    front_own = front_grad(grads_own) + grad_came.astype(F32)
    unit_one = own["inputs"] * own["scale"]
    attn_gain_grad = jnp.sum(front_own * unit_one, axis=0)
    unit_grad = front_own * attn_gain_all
    input_grad = residual_grad[:rows] + own["scale"] * (
        unit_grad - unit_one * jnp.mean(unit_grad * unit_one, axis=-1, keepdims=True)
    )

    normed_both = jnp.concatenate([own["normed"], oth["normed"]])
    joined = jnp.concatenate(
        [jnp.concatenate([a, b]) for a, b in zip(grads_own, grads_oth)], axis=1
    )
    projections = sum_over_rep(mm_tn(joined, normed_both).astype(BF16), straight, me, n_rep)
    cut = query_weight.shape[0], query_weight.shape[0] + key_weight.shape[0]

    attn_gain_grad = half_of(attn_gain_grad, g, 0) + swap(half_of(attn_gain_grad, 1 - g, 0))
    small = jnp.concatenate(
        [a + b for a, b in zip(sums_own, sums_oth)] + [attn_gain_grad, half_of(mlp_gain_grad, g, 0)]
    )
    small = lax.psum(small, "rep")
    edges = [0]
    for piece in (query_bias, key_bias, value_bias, attn_gain, mlp_gain):
        edges.append(edges[-1] + piece.shape[0])
    pieces = [small[a:b] for a, b in zip(edges, edges[1:])]
    return (
        block_out,
        input_grad,
        projections[: cut[0]],
        projections[cut[0] : cut[1]],
        projections[cut[1] :],
        pieces[0],
        pieces[1],
        pieces[2],
        output_weight_grad,
        gate_weight_grad,
        up_weight_grad,
        down_weight_grad,
        pieces[3],
        pieces[4],
    )


def solution(mesh):
    n_rep = mesh.shape["rep"]
    assert mesh.shape["grp"] == 2 and n_rep & (n_rep - 1) == 0
    rows = P(("rep", "grp"), None)
    wide, flat = P("grp", None), P("grp")
    return jax.shard_map(
        lambda *args: local(n_rep, *args),
        mesh=mesh,
        in_specs=(rows, wide, wide, wide, flat, flat, flat, wide, wide, wide, wide, flat, flat, rows, rows),
        out_specs=(rows, rows, wide, wide, wide, flat, flat, flat, wide, wide, wide, wide, flat, flat),
        check_vma=False,
    )
```

```python
import functools
import math

import jax
import jax.numpy as jnp
from jax import lax
from jax.experimental import pallas as pl
from jax.experimental.pallas import tpu as pltpu
from jax.sharding import PartitionSpec as P

QUERY_HEADS = 12
KEY_VALUE_HEADS = 2
HEAD_SIZE = 128

EPSILON = 1e-06
THETA = 1000000.0

BF16 = jnp.bfloat16
F32 = jnp.float32
MESH = pl.DeviceIdType.MESH


def contract(form, left, right):
    return jnp.einsum(form, left, right, preferred_element_type=F32)


def mm_nt(left, right):
    return lax.dot_general(left, right, (((1,), (1,)), ((), ())), preferred_element_type=F32)


def mm_nn(left, right):
    return lax.dot_general(left, right, (((1,), (0,)), ((), ())), preferred_element_type=F32)


def mm_tn(left, right):
    return lax.dot_general(left, right, (((0,), (0,)), ((), ())), preferred_element_type=F32)


def layout(seq_lengths, count_of_rows):
    seq_ends = jnp.cumsum(seq_lengths)
    seq_starts = seq_ends - seq_lengths
    row_index = jnp.arange(count_of_rows, dtype=jnp.int32)
    segment = jnp.sum((row_index[:, None] >= seq_ends[None, :]).astype(jnp.int32), axis=1)
    member = segment[:, None] == jnp.arange(seq_lengths.shape[0], dtype=jnp.int32)[None, :]
    position = row_index - jnp.sum(jnp.where(member, seq_starts[None, :], 0), axis=1)
    allowed = (segment[:, None] == segment[None, :]) & (row_index[None, :] <= row_index[:, None])
    return (position, allowed)


def rotary_tables(position, head_dim):
    half_dim = head_dim // 2
    exponent = jnp.arange(half_dim, dtype=F32) * (2.0 / head_dim)
    frequency = jnp.exp(-exponent * math.log(THETA))
    angles = position.astype(F32)[:, None] * frequency[None, :]
    cosine = jnp.cos(angles)
    sine = jnp.sin(angles)
    return (jnp.concatenate([cosine, cosine], axis=-1), jnp.concatenate([sine, sine], axis=-1))


def apply_rotary(vectors, cosine, sine):
    half_dim = vectors.shape[-1] // 2
    turned = jnp.concatenate([-vectors[..., half_dim:], vectors[..., :half_dim]], axis=-1)
    return vectors * cosine[:, None, :] + turned * sine[:, None, :]


def inverse_rotary(grads, cosine, sine):
    half_dim = grads.shape[-1] // 2
    scaled = grads * sine[:, None, :]
    turned = jnp.concatenate([scaled[..., half_dim:], -scaled[..., :half_dim]], axis=-1)
    return grads * cosine[:, None, :] + turned


def rms_scale(values):
    return lax.rsqrt(jnp.mean(values * values, axis=-1, keepdims=True) + EPSILON)


def swap(x):
    return lax.ppermute(x, "grp", [(0, 1), (1, 0)])


def after(x, earlier):
    return lax.optimization_barrier((x, earlier))[0]


def swap_shared(x, n_rep):
    odd = lax.axis_index("rep") & 1
    came = swap(half_of(x, odd, 0))
    shared = lax.ppermute(came, "rep", [(i, i ^ 1) for i in range(n_rep)])
    return in_order(came, shared, odd)


def in_order(mine, other, g, axis=0):
    first = jnp.where(g == 0, mine, other)
    second = jnp.where(g == 0, other, mine)
    return jnp.concatenate([first, second], axis)


def half_of(x, which, axis):
    size = x.shape[axis] // 2
    return lax.dynamic_slice_in_dim(x, which * size, size, axis)


def rows_loop(count, step, body):
    def one(i, carry):
        body(pl.multiple_of(i * step, step), step)
        return carry

    lax.fori_loop(0, count // step, one, 0)


def pool_kernel(plan, groups, n_rep, *refs):
    n_parts = sum(len(parts) for _, parts, _ in groups)
    ins, (small_ref, out_ref, small_out) = refs[:n_parts], refs[n_parts : n_parts + 3]
    pool, full, inbox, small_box, in_sem, out_sem, send_sem, recv_sem, small_send, small_recv = refs[n_parts + 3 :]
    me, g = lax.axis_index("rep"), lax.axis_index("grp")
    bits = n_rep.bit_length() - 1
    half = pool.shape[1] // 2

    barrier = pltpu.get_barrier_semaphore()
    for b in range(bits):
        pl.semaphore_signal(barrier, inc=1, device_id={"rep": me ^ (1 << b)}, device_id_type=MESH)
    pl.semaphore_signal(barrier, inc=1, device_id={"grp": 1 - g}, device_id_type=MESH)

    loads, at = [], 0
    for base, parts, end in groups:
        loads.append([])
        for count in parts:
            loads[-1].append(pltpu.make_async_copy(ins[at], pool.at[pl.ds(base, count)], in_sem.at[at]))
            loads[-1][-1].start()
            base, at = base + count, at + 1
        if base < end:
            pool[pl.ds(base, end - base), :] = jnp.zeros((end - base, pool.shape[1]), BF16)
    small_box[0] = small_ref[...]
    pl.semaphore_wait(barrier, bits + 1)

    copies, state, box_at, used = {}, {}, {}, 0
    for u, (start, size, order, group, cross) in enumerate(plan):
        n = size
        for s in range(bits):
            n //= 2
            box_at[u, s] = used
            used += n
    loaded = set()
    numbers = {}

    def remote(source, target, key, there):
        at = numbers.setdefault(key, len(numbers))
        copies[key] = pltpu.make_async_remote_copy(
            src_ref=source,
            dst_ref=target,
            send_sem=send_sem.at[at],
            recv_sem=recv_sem.at[at],
            device_id=there,
            device_id_type=MESH,
        )
        copies[key].start()

    def bit_of(b):
        return (me >> b) & 1

    def advance(u, step):
        start, size, order, group, cross = plan[u]
        kinds = ["halve"] * bits + ["cross"] * cross + ["double"] * bits + ["out"]
        if step == 0:
            if group not in loaded:
                loaded.add(group)
                for load in loads[group]:
                    load.wait()
            state[u] = [jnp.int32(start), size]
        else:
            copies[u, step - 1].wait()
            before = kinds[step - 1]
            off, n = state[u]
            if before == "halve":
                n //= 2
                at = box_at[u, step - 1]
                keep = pl.multiple_of(off + bit_of(order[step - 1]) * n, n)
                target = full if kinds[step] == "double" else pool

                def add(i, count):
                    there = pl.ds(pl.multiple_of(keep + i, 16), count)
                    here = pl.ds(pl.multiple_of(at + i, 16), count)
                    target[there, :] = (pool[there, :].astype(F32) + inbox[here, :].astype(F32)).astype(BF16)

                rows_loop(n, 16 if n % 32 else 32, add)
                state[u] = [keep, n]
            elif before == "double":
                b = order[2 * bits + cross - step]
                state[u] = [pl.multiple_of(off - bit_of(b) * n, n), 2 * n]
        off, n = state[u]
        kind = kinds[step]
        if kind == "halve":
            n //= 2
            b = order[step]
            give = pl.multiple_of(off + (1 - bit_of(b)) * n, n)
            target = inbox.at[pl.ds(box_at[u, step], n)]
            remote(pool.at[pl.ds(give, n)], target, (u, step), {"rep": me ^ (1 << b)})
        elif kind == "cross":
            rows = pl.ds(off, n)
            mine = pl.ds(pl.multiple_of(g * half, 128), half)
            theirs = pl.ds(pl.multiple_of((1 - g) * half, 128), half)
            remote(pool.at[rows, theirs], full.at[rows, mine], (u, step), {"grp": 1 - g})
            full[rows, mine] = pool[rows, mine]
        elif kind == "double":
            b = order[2 * bits + cross - 1 - step]
            block = pl.ds(off, n)
            remote(full.at[block], full.at[block], (u, step), {"rep": me ^ (1 << b)})
        else:
            rows = pl.ds(start, size)
            copies[u, step] = pltpu.make_async_copy(full.at[rows], out_ref.at[rows], out_sem.at[u])
            copies[u, step].start()

    def advance_small(s):
        if s > 0:
            copies["small", s - 1].wait()
            if s <= bits:
                small_box[2 * s] = small_box[2 * s - 2] + small_box[2 * s - 1]
        if s <= bits:
            copies["small", s] = pltpu.make_async_remote_copy(
                src_ref=small_box.at[2 * s],
                dst_ref=small_box.at[2 * s + 1],
                send_sem=small_send.at[s],
                recv_sem=small_recv.at[s],
                device_id={"rep": me ^ (1 << s)} if s < bits else {"grp": 1 - g},
                device_id_type=MESH,
            )
            copies["small", s].start()
        else:
            small_out[0] = small_box[2 * bits]
            small_out[1] = small_box[2 * bits + 1]

    steps = [2 * bits + 1 + cross for *_, cross in plan]
    for t in range(max(u + n for u, n in enumerate(steps))):
        for u in range(len(plan)):
            if 0 <= t - u < steps[u]:
                advance(u, t - u)
        if t <= bits + 1:
            advance_small(t)
    for u in range(len(plan)):
        copies[u, steps[u] - 1].wait()


def sum_pool(groups, small, n_rep):
    bits = n_rep.bit_length() - 1
    straight = tuple(range(bits))
    crossed = (0, 2, 1) + tuple(range(3, bits)) if bits >= 3 else straight
    grain = 16 * n_rep
    unit = max(768 // grain, 1) * grain
    flat = [a for arrays, _ in groups for a in arrays]
    width = flat[0].shape[1]
    plan, places, base = [], [], 0
    for k, (arrays, cross) in enumerate(groups):
        counts = [a.shape[0] for a in arrays]
        end = base + -(-sum(counts) // grain) * grain
        places.append((base, counts, end))
        for start in range(base, end, unit):
            order = crossed if len(plan) % 4 == 2 else straight
            plan.append((start, min(unit, end - start), order, k, int(cross)))
        base = end
    box = sum(size - size // n_rep for _, size, *_ in plan)
    n_copies = sum(2 * bits + cross for *_, cross in plan)
    any_space = pl.BlockSpec(memory_space=pl.ANY)
    vmem = pl.BlockSpec(memory_space=pltpu.VMEM)
    pool, sums = pl.pallas_call(
        functools.partial(pool_kernel, plan, places, n_rep),
        out_shape=(jax.ShapeDtypeStruct((base, width), BF16), jax.ShapeDtypeStruct((2,) + small.shape, F32)),
        in_specs=[any_space] * len(flat) + [vmem],
        out_specs=(any_space, vmem),
        scratch_shapes=[
            pltpu.VMEM((base, width), BF16),
            pltpu.VMEM((base, width), BF16),
            pltpu.VMEM((box, width), BF16),
            pltpu.VMEM((2 * bits + 2,) + small.shape, F32),
            pltpu.SemaphoreType.DMA((len(flat),)),
            pltpu.SemaphoreType.DMA((len(plan),)),
            pltpu.SemaphoreType.DMA((n_copies,)),
            pltpu.SemaphoreType.DMA((n_copies,)),
            pltpu.SemaphoreType.DMA((bits + 1,)),
            pltpu.SemaphoreType.DMA((bits + 1,)),
        ],
        compiler_params=pltpu.CompilerParams(
            collective_id=0, has_side_effects=True, vmem_limit_bytes=60 * 1024 * 1024
        ),
    )(*flat, small)
    pieces = []
    for base, counts, _ in places:
        for count in counts:
            pieces.append(pool[base : base + count])
            base += count
    return pieces, sums


def ffn_kernel(n2, cot, gate, up, down, hid_out, gg_out, ug_out, ng_out, ngb_out, dp_out, ng_acc, dp_acc):
    step = pl.program_id(0)

    @pl.when(step == 0)
    def _():
        ng_acc[...] = jnp.zeros_like(ng_acc)
        dp_acc[...] = jnp.zeros_like(dp_acc)

    gate_pre = mm_nt(gate[...], n2[...])
    up_proj = mm_nt(up[...], n2[...])
    hidden_grad = mm_nt(down[...], cot[...])
    sigmoid = 1.0 / (1.0 + jnp.exp(-gate_pre))
    activated = gate_pre * sigmoid
    hidden = (activated * up_proj).astype(BF16)
    gate_grad = (hidden_grad * up_proj * sigmoid * (1.0 + gate_pre * (1.0 - sigmoid))).astype(BF16)
    up_grad = (hidden_grad * activated).astype(BF16)
    hid_out[...] = hidden
    gg_out[...] = gate_grad
    ug_out[...] = up_grad
    ng_acc[...] += mm_tn(gate_grad, gate[...]) + mm_tn(up_grad, up[...])
    dp_acc[...] += mm_tn(hidden, down[...])

    @pl.when(step == pl.num_programs(0) - 1)
    def _():
        ng_out[...] = ng_acc[...]
        ngb_out[...] = ng_acc[...].astype(BF16)
        dp_out[...] = dp_acc[...].astype(dp_out.dtype)


def block_of(count, limit, grain):
    return max(d for d in range(grain, limit + 1, grain) if count % d == 0)


def ffn(n2, cot, gate, up, down, part_type):
    rows, width = n2.shape
    units = gate.shape[0]
    block = block_of(units, 512, 16)
    whole = pl.BlockSpec((rows, width), lambda i: (0, 0))
    cut = pl.BlockSpec((block, width), lambda i: (i, 0))
    cut_rows = pl.BlockSpec((block, rows), lambda i: (i, 0))
    wide = jax.ShapeDtypeStruct((units, rows), BF16)
    return pl.pallas_call(
        ffn_kernel,
        grid=(units // block,),
        out_shape=(
            wide,
            wide,
            wide,
            jax.ShapeDtypeStruct((rows, width), F32),
            jax.ShapeDtypeStruct((rows, width), BF16),
            jax.ShapeDtypeStruct((rows, width), part_type),
        ),
        in_specs=[whole, whole, cut, cut, cut],
        out_specs=(cut_rows, cut_rows, cut_rows, whole, whole, whole),
        scratch_shapes=[pltpu.VMEM((rows, width), F32), pltpu.VMEM((rows, width), F32)],
        compiler_params=pltpu.CompilerParams(vmem_limit_bytes=56 * 1024 * 1024),
        cost_estimate=pl.CostEstimate(
            flops=12 * units * rows * width, bytes_accessed=12 * units * width, transcendentals=units * rows
        ),
    )(n2, cot, gate, up, down)


def grads_kernel(hid_a, gg_a, ug_a, hid_b, gg_b, ug_b, n2_a, n2_b, cot_a, cot_b, dw, gw, uw):
    dw[...] = (mm_nn(hid_a[...], cot_a[...]) + mm_nn(hid_b[...], cot_b[...])).astype(BF16)
    gw[...] = (mm_nn(gg_a[...], n2_a[...]) + mm_nn(gg_b[...], n2_b[...])).astype(BF16)
    uw[...] = (mm_nn(ug_a[...], n2_a[...]) + mm_nn(ug_b[...], n2_b[...])).astype(BF16)


def ffn_grads(first, second, n2, cot):
    units, rows = first[0].shape
    width = n2[0].shape[1]
    block = block_of(units, 512, 16)
    whole = pl.BlockSpec((rows, width), lambda i: (0, 0))
    cut = pl.BlockSpec((block, width), lambda i: (i, 0))
    cut_rows = pl.BlockSpec((block, rows), lambda i: (i, 0))
    return pl.pallas_call(
        grads_kernel,
        grid=(units // block,),
        out_shape=(jax.ShapeDtypeStruct((units, width), BF16),) * 3,
        in_specs=[cut_rows] * 6 + [whole] * 4,
        out_specs=(cut,) * 3,
        compiler_params=pltpu.CompilerParams(vmem_limit_bytes=56 * 1024 * 1024),
        cost_estimate=pl.CostEstimate(
            flops=12 * units * rows * width, bytes_accessed=18 * units * width, transcendentals=0
        ),
    )(*first, *second, *n2, *cot)


def attention_forward(query_rotated, key_rotated, values, allowed):
    scores = contract("thd,sd->hts", query_rotated, key_rotated) * (1.0 / math.sqrt(HEAD_SIZE))
    scores = jnp.where(allowed, scores, -1e30)
    row_peak = jnp.max(scores, axis=-1, keepdims=True)
    log_total = row_peak + jnp.log(jnp.sum(jnp.exp(scores - row_peak), axis=-1, keepdims=True))
    probs = jnp.exp(scores - log_total).astype(BF16)
    mixed = contract("hts,sd->thd", probs, values)
    return mixed.reshape(mixed.shape[0], -1).astype(BF16), log_total


def attention_backward(query_rotated, key_rotated, values, allowed, log_total, mixed, mixed_grad):
    heads = query_rotated.shape[1]
    rows = query_rotated.shape[0]
    score_scale = 1.0 / math.sqrt(HEAD_SIZE)
    mixed = mixed.reshape(rows, heads, HEAD_SIZE)
    mixed_grad = mixed_grad.reshape(rows, heads, HEAD_SIZE)
    scores = contract("thd,sd->hts", query_rotated, key_rotated) * score_scale
    scores = jnp.where(allowed, scores, -1e30)
    probs = jnp.exp(scores - log_total)
    values_grad = contract("hts,thd->sd", probs.astype(BF16), mixed_grad)
    probs_grad = contract("thd,sd->hts", mixed_grad, values)
    delta = jnp.sum(mixed_grad.astype(F32) * mixed.astype(F32), axis=-1)
    delta = jnp.transpose(delta, (1, 0))[..., None]
    score_grad = (probs * (probs_grad - delta) * score_scale).astype(BF16)
    queries_grad = contract("hts,sd->thd", score_grad, key_rotated)
    keys_grad = contract("hts,thd->sd", score_grad, query_rotated)
    return queries_grad, keys_grad, values_grad


def local(
    n_rep,
    tokens,
    query_weight,
    key_weight,
    value_weight,
    query_bias,
    key_bias,
    value_bias,
    output_matrix,
    gate_weight,
    up_weight,
    down_weight,
    attn_gain,
    mlp_gain,
    cotangent,
    seq_lengths,
):
    g = lax.axis_index("grp")
    rows = tokens.shape[0]
    heads = query_weight.shape[0] // HEAD_SIZE

    gains = jnp.stack([attn_gain, mlp_gain])
    gains_other = swap(gains)
    tokens_other = swap(tokens)
    lengths_other = swap(seq_lengths)
    output_other = swap_shared(after(half_of(output_matrix, 1 - g, 1), tokens_other), n_rep)
    cotangent_other = swap(after(cotangent, output_other))
    down_other = swap_shared(after(half_of(down_weight, 1 - g, 1), cotangent_other), n_rep)
    gains = in_order(gains, gains_other, g, 1).astype(F32)
    attn_gain_all, mlp_gain_all = gains[0:1], gains[1:2]
    output_cols = in_order(half_of(output_matrix, g, 1), output_other, g)
    down_rows = in_order(half_of(down_weight, g, 1), down_other, g).T

    def front(token_rows, lengths):
        position, allowed = layout(lengths[0], rows)
        cosine, sine = rotary_tables(position, HEAD_SIZE)
        inputs = token_rows.astype(F32)
        scale = rms_scale(inputs)
        normed = (inputs * scale * attn_gain_all).astype(BF16)
        queries = mm_nt(normed, query_weight) + query_bias.astype(F32)
        keys = mm_nt(normed, key_weight) + key_bias.astype(F32)
        values = (mm_nt(normed, value_weight) + value_bias.astype(F32)).astype(BF16)
        queries = apply_rotary(queries.reshape(rows, heads, HEAD_SIZE), cosine, sine).astype(BF16)
        keys = apply_rotary(keys[:, None, :], cosine, sine)[:, 0].astype(BF16)
        mixed, log_total = attention_forward(queries, keys, values, allowed)
        part = mm_nt(mixed, output_cols)
        return dict(
            inputs=inputs,
            scale=scale,
            normed=normed,
            queries=queries,
            keys=keys,
            values=values,
            mixed=mixed,
            log_total=log_total,
            part=part,
            allowed=allowed,
            cosine=cosine,
            sine=sine,
        )

    own = front(tokens, seq_lengths)
    came_other = swap(own["part"].astype(BF16))
    oth = front(tokens_other, lengths_other)
    came_own = swap(oth["part"].astype(BF16))
    def middle(kept, came, cot, part_type):
        residual = kept["inputs"] + kept["part"] + came.astype(F32)
        scale = rms_scale(residual)
        normed = (residual * scale * mlp_gain_all).astype(BF16)
        *wide, grad, grad_b, part = ffn(normed, cot, gate_weight, up_weight, down_rows, part_type)
        return dict(residual=residual, scale=scale, normed=normed, wide=wide, grad=grad, grad_b=grad_b, part=part)

    mid_oth = middle(oth, came_other, cotangent_other, BF16)
    grad_came_own = swap(mid_oth["grad_b"])
    mid_own = middle(own, came_own, cotangent, F32)
    grad_came_oth = swap(after(mid_own["grad_b"], grad_came_own))
    down_came = swap(after(mid_oth["part"], grad_came_oth))
    block_out = mid_own["residual"] + mid_own["part"] + down_came.astype(F32)
    down_grad, gate_weight_grad, up_weight_grad = ffn_grads(
        mid_oth["wide"],
        mid_own["wide"],
        (mid_oth["normed"], mid_own["normed"]),
        (cotangent_other, cotangent),
    )

    def middle_grad(mid, came, cot):
        normed_grad = mid["grad"] + came.astype(F32)
        unit = mid["residual"] * mid["scale"]
        gain_grad = jnp.sum(normed_grad * unit, axis=0)
        unit_grad = normed_grad * mlp_gain_all
        residual_grad = cot.astype(F32) + mid["scale"] * (
            unit_grad - unit * jnp.mean(unit_grad * unit, axis=-1, keepdims=True)
        )
        return residual_grad, residual_grad.astype(BF16), gain_grad

    residual_grad_own, residual_grad_own_b, gain_grad_own = middle_grad(mid_own, grad_came_own, cotangent)
    residual_grad_oth, residual_grad_oth_b, gain_grad_oth = middle_grad(mid_oth, grad_came_oth, cotangent_other)
    mlp_gain_grad = gain_grad_own + gain_grad_oth

    residual_grad_b = jnp.concatenate([residual_grad_own_b, residual_grad_oth_b])
    mixed_both = jnp.concatenate([own["mixed"], oth["mixed"]])
    output_grad = mm_tn(mixed_both, residual_grad_b).astype(BF16)
    mixed_grad_own = mm_nn(residual_grad_own_b, output_cols).astype(BF16)
    mixed_grad_oth = mm_nn(residual_grad_oth_b, output_cols).astype(BF16)

    def back(kept, mixed_grad):
        queries_grad, keys_grad, values_grad = attention_backward(
            kept["queries"],
            kept["keys"],
            kept["values"],
            kept["allowed"],
            kept["log_total"],
            kept["mixed"],
            mixed_grad,
        )
        queries_grad = inverse_rotary(queries_grad, kept["cosine"], kept["sine"]).reshape(rows, -1)
        keys_grad = inverse_rotary(keys_grad[:, None, :], kept["cosine"], kept["sine"])[:, 0]
        sums = (jnp.sum(queries_grad, 0), jnp.sum(keys_grad, 0), jnp.sum(values_grad, 0))
        return sums, (queries_grad.astype(BF16), keys_grad.astype(BF16), values_grad.astype(BF16))

    def front_grad(grads):
        queries_b, keys_b, values_b = grads
        return mm_nn(queries_b, query_weight) + mm_nn(keys_b, key_weight) + mm_nn(values_b, value_weight)

    sums_oth, grads_oth = back(oth, mixed_grad_oth)
    front_oth = front_grad(grads_oth)
    front_came = swap(after(front_oth.astype(BF16), down_came))
    sums_own, grads_own = back(own, mixed_grad_own)
    front_own = front_grad(grads_own)
    unit_one = own["inputs"] * own["scale"]
    attn_gain_grad = jnp.sum(front_own * unit_one + front_oth * (oth["inputs"] * oth["scale"]), axis=0)
    front_own = front_own + front_came.astype(F32)
    unit_grad = front_own * attn_gain_all
    input_grad = residual_grad_own + own["scale"] * (
        unit_grad - unit_one * jnp.mean(unit_grad * unit_one, axis=-1, keepdims=True)
    )

    normed_both = jnp.concatenate([own["normed"], oth["normed"]])
    joined = jnp.concatenate(
        [jnp.concatenate([a, b]) for a, b in zip(grads_own, grads_oth)], axis=1
    )
    projections = mm_tn(joined, normed_both).astype(BF16)

    small = jnp.concatenate(
        [a + b for a, b in zip(sums_own, sums_oth)] + [half_of(mlp_gain_grad, g, 0), attn_gain_grad]
    )
    count = small.shape[0]
    lines = -(-count // (8 * 128)) * 8
    small = jnp.pad(small, (0, lines * 128 - count)).reshape(lines, 128)
    pieces, small = sum_pool(
        [([down_grad], True), ([gate_weight_grad, up_weight_grad], False), ([output_grad], True), ([projections], False)],
        small,
        n_rep,
    )
    small = small.reshape(2, -1)
    vectors, at = [], 0
    for piece in (query_bias, key_bias, value_bias, mlp_gain):
        vectors.append(small[0, at : at + piece.shape[0]])
        at += piece.shape[0]
    vectors.append(half_of(small[0, at:count] + small[1, at:count], g, 0))
    half = down_grad.shape[1] // 2

    def owned(piece):
        return jnp.concatenate([piece[:, :half].T, piece[:, half:].T], axis=1).astype(F32)

    down_weight_grad, output_weight_grad = owned(pieces[0]), owned(pieces[3])
    gate_weight_grad, up_weight_grad = pieces[1].astype(F32), pieces[2].astype(F32)
    cut = query_weight.shape[0], query_weight.shape[0] + key_weight.shape[0]
    projections = pieces[4]
    return (
        block_out,
        input_grad,
        projections[: cut[0]].astype(F32),
        projections[cut[0] : cut[1]].astype(F32),
        projections[cut[1] :].astype(F32),
        vectors[0],
        vectors[1],
        vectors[2],
        output_weight_grad,
        gate_weight_grad,
        up_weight_grad,
        down_weight_grad,
        vectors[4],
        vectors[3],
    )


def solution(mesh):
    n_rep = mesh.shape["rep"]
    assert mesh.shape["grp"] == 2 and n_rep & (n_rep - 1) == 0
    rows = P(("rep", "grp"), None)
    wide, flat = P("grp", None), P("grp")
    return jax.shard_map(
        lambda *args: local(n_rep, *args),
        mesh=mesh,
        in_specs=(rows, wide, wide, wide, flat, flat, flat, wide, wide, wide, wide, flat, flat, rows, rows),
        out_specs=(rows, rows, wide, wide, wide, flat, flat, flat, wide, wide, wide, wide, flat, flat),
        check_vma=False,
    )
```

```python
import functools
import math

import jax
import jax.numpy as jnp
from jax import lax
from jax.experimental import pallas as pl
from jax.experimental.pallas import tpu as pltpu
from jax.sharding import PartitionSpec as P


HEAD_SIZE = 128

EPSILON = 1e-06
THETA = 1000000.0

BF16 = jnp.bfloat16
F32 = jnp.float32
MESH = pl.DeviceIdType.MESH


def mm_nt(left, right):
    return lax.dot_general(left, right, (((1,), (1,)), ((), ())), preferred_element_type=F32)


def mm_nn(left, right):
    return lax.dot_general(left, right, (((1,), (0,)), ((), ())), preferred_element_type=F32)


def mm_tn(left, right):
    return lax.dot_general(left, right, (((0,), (0,)), ((), ())), preferred_element_type=F32)


def rotary_tables(position, head_dim):
    half_dim = head_dim // 2
    exponent = jnp.arange(half_dim, dtype=F32) * (2.0 / head_dim)
    frequency = jnp.exp(-exponent * math.log(THETA))
    angles = position.astype(F32)[:, None] * frequency[None, :]
    cosine = jnp.cos(angles)
    sine = jnp.sin(angles)
    return (jnp.concatenate([cosine, cosine], axis=-1), jnp.concatenate([sine, sine], axis=-1))


def rms_scale(values):
    return lax.rsqrt(jnp.mean(values * values, axis=-1, keepdims=True) + EPSILON)


def swap(x):
    return lax.ppermute(x, "grp", [(0, 1), (1, 0)])


def after(x, earlier):
    return lax.optimization_barrier((x, earlier))[0]


def swap_shared(x, n_rep, levels=2):
    levels = min(levels, n_rep.bit_length() - 1)
    me = lax.axis_index("rep")
    count = x.shape[0] >> levels
    came = swap(lax.dynamic_slice_in_dim(x, (me & ((1 << levels) - 1)) * count, count, 0))
    for b in range(levels):
        shared = lax.ppermute(came, "rep", [(i, i ^ (1 << b)) for i in range(n_rep)])
        came = in_order(came, shared, (me >> b) & 1)
    return came


def in_order(mine, other, g, axis=0):
    first = jnp.where(g == 0, mine, other)
    second = jnp.where(g == 0, other, mine)
    return jnp.concatenate([first, second], axis)


def half_of(x, which, axis):
    size = x.shape[axis] // 2
    return lax.dynamic_slice_in_dim(x, which * size, size, axis)


def rows_loop(count, step, body):
    def one(i, carry):
        body(pl.multiple_of(i * step, step), step)
        return carry

    lax.fori_loop(0, count // step, one, 0)


def pool_kernel(plan, groups, n_rep, *refs):
    n_parts = sum(len(parts) for _, parts, *_ in groups)
    n_outs = sum(1 if cross else len(cuts) for _, _, _, cuts, cross in groups)
    ins, small_ref, refs = refs[:n_parts], refs[n_parts], refs[n_parts + 1 :]
    outs, small_out, refs = refs[:n_outs], refs[n_outs], refs[n_outs + 1 :]
    pool, full, inbox, flipped, small_box, in_sem, out_sem, send_sem, recv_sem, small_send, small_recv = refs
    me, g = lax.axis_index("rep"), lax.axis_index("grp")
    bits = n_rep.bit_length() - 1
    half = pool.shape[1] // 2

    barrier = pltpu.get_barrier_semaphore()
    for b in range(bits):
        pl.semaphore_signal(barrier, inc=1, device_id={"rep": me ^ (1 << b)}, device_id_type=MESH)
    pl.semaphore_signal(barrier, inc=1, device_id={"grp": 1 - g}, device_id_type=MESH)

    loads, at = [], 0
    for base, parts, end, *_ in groups:
        loads.append([])
        for count in parts:
            loads[-1].append(pltpu.make_async_copy(ins[at], pool.at[pl.ds(base, count)], in_sem.at[at]))
            loads[-1][-1].start()
            base, at = base + count, at + 1
        if base < end:
            pool[pl.ds(base, end - base), :] = jnp.zeros((end - base, pool.shape[1]), BF16)
    small_box[0] = small_ref[...]
    pl.semaphore_wait(barrier, bits + 1)

    copies, state, box_at, used = {}, {}, {}, 0
    for u, (start, size, order, group, cross) in enumerate(plan):
        n = size
        for s in range(bits):
            n //= 2
            box_at[u, s] = used
            used += n
    loaded, numbers, leaving, flips, count_of_flips = set(), {}, [], [], [0]

    def remote(source, target, key, there):
        at = numbers.setdefault(key, len(numbers))
        copies[key] = pltpu.make_async_remote_copy(
            src_ref=source,
            dst_ref=target,
            send_sem=send_sem.at[at],
            recv_sem=recv_sem.at[at],
            device_id=there,
            device_id_type=MESH,
        )
        copies[key].start()

    def bit_of(b):
        return (me >> b) & 1

    def advance(u, step):
        start, size, order, group, cross = plan[u]
        kinds = ["halve"] * bits + ["cross"] * cross + ["double"] * bits + ["out"]
        if step == 0:
            if group not in loaded:
                loaded.add(group)
                for load in loads[group]:
                    load.wait()
            state[u] = [jnp.int32(start), size]
        else:
            copies[u, step - 1].wait()
            before = kinds[step - 1]
            off, n = state[u]
            if before == "halve":
                n //= 2
                at = box_at[u, step - 1]
                keep = pl.multiple_of(off + bit_of(order[step - 1]) * n, n)
                target = full if kinds[step] == "double" else pool

                def add(i, count):
                    there = pl.ds(pl.multiple_of(keep + i, 16), count)
                    here = pl.ds(pl.multiple_of(at + i, 16), count)
                    target[there, :] = (pool[there, :].astype(F32) + inbox[here, :].astype(F32)).astype(BF16)

                rows_loop(n, 16 if n % 32 else 32, add)
                state[u] = [keep, n]
            elif before == "double":
                b = order[2 * bits + cross - step]
                state[u] = [pl.multiple_of(off - bit_of(b) * n, n), 2 * n]
        off, n = state[u]
        kind = kinds[step]
        if kind == "halve":
            n //= 2
            b = order[step]
            give = pl.multiple_of(off + (1 - bit_of(b)) * n, n)
            target = inbox.at[pl.ds(box_at[u, step], n)]
            remote(pool.at[pl.ds(give, n)], target, (u, step), {"rep": me ^ (1 << b)})
        elif kind == "cross":
            rows = pl.ds(off, n)
            mine = pl.ds(pl.multiple_of(g * half, 128), half)
            theirs = pl.ds(pl.multiple_of((1 - g) * half, 128), half)
            remote(pool.at[rows, theirs], full.at[rows, mine], (u, step), {"grp": 1 - g})
            full[rows, mine] = pool[rows, mine]
        elif kind == "double":
            b = order[2 * bits + cross - 1 - step]
            block = pl.ds(off, n)
            remote(full.at[block], full.at[block], (u, step), {"rep": me ^ (1 << b)})
        else:
            first = sum(1 if c else len(cuts) for _, _, _, cuts, c in groups[:group])
            base, _, _, cuts, _ = groups[group]
            wanted = []
            if cross:
                slot = count_of_flips[0] % 2
                if count_of_flips[0] > 1:
                    flips[count_of_flips[0] - 2].wait()
                count_of_flips[0] += 1

                def flip(i, count):
                    piece = full[pl.ds(pl.multiple_of(start + i, 128), count), :].astype(F32)
                    flipped[slot, :, pl.ds(pl.multiple_of(i, 128), count)] = piece.T.astype(BF16)

                rows_loop(size, 128, flip)
                wanted.append((flipped.at[slot, :, pl.ds(0, size)], outs[first].at[:, pl.ds(start - base, size)]))
            for k, count in enumerate(() if cross else cuts):
                low, high = max(base, start), min(base + count, start + size)
                if low < high:
                    wanted.append((full.at[pl.ds(low, high - low)], outs[first + k].at[pl.ds(low - base, high - low)]))
                base += count
            for source, target in wanted:
                copy = pltpu.make_async_copy(source, target, out_sem.at[len(leaving) + len(flips)])
                copy.start()
                (flips if cross else leaving).append(copy)

    def advance_small(s):
        if s > 0:
            copies["small", s - 1].wait()
            if s <= bits:
                small_box[2 * s] = small_box[2 * s - 2] + small_box[2 * s - 1]
        if s <= bits:
            copies["small", s] = pltpu.make_async_remote_copy(
                src_ref=small_box.at[2 * s],
                dst_ref=small_box.at[2 * s + 1],
                send_sem=small_send.at[s],
                recv_sem=small_recv.at[s],
                device_id={"rep": me ^ (1 << s)} if s < bits else {"grp": 1 - g},
                device_id_type=MESH,
            )
            copies["small", s].start()
        else:
            small_out[0] = small_box[2 * bits]
            small_out[1] = small_box[2 * bits + 1]

    steps = [2 * bits + 1 + cross for *_, cross in plan]
    for t in range(max(u + n for u, n in enumerate(steps))):
        for u in range(len(plan)):
            if 0 <= t - u < steps[u]:
                advance(u, t - u)
        if t <= bits + 1:
            advance_small(t)
    for copy in leaving + flips[-2:]:
        copy.wait()


def sum_pool(groups, small, n_rep):
    bits = n_rep.bit_length() - 1
    straight = tuple(range(bits))
    crossed = (0, 2, 1) + tuple(range(3, bits)) if bits >= 3 else straight
    grain = 16 * n_rep
    unit = max(768 // grain, 1) * grain
    flat = [a for arrays, _, _ in groups for a in arrays]
    width = flat[0].shape[1]
    plan, places, outs, base = [], [], [], 0
    for k, (arrays, cuts, cross) in enumerate(groups):
        counts = [a.shape[0] for a in arrays]
        end = base + -(-sum(counts) // grain) * grain
        places.append((base, counts, end, cuts, cross))
        for start in range(base, end, unit):
            order = crossed if len(plan) % 4 == 2 else straight
            plan.append((start, min(unit, end - start), order, k, int(cross)))
        outs += [(width, end - base)] if cross else [(count, width) for count in cuts]
        base = end
    box = sum(size - size // n_rep for _, size, *_ in plan)
    n_copies = sum(2 * bits + cross for *_, cross in plan)
    any_space = pl.BlockSpec(memory_space=pl.ANY)
    vmem = pl.BlockSpec(memory_space=pltpu.VMEM)
    *pieces, sums = pl.pallas_call(
        functools.partial(pool_kernel, plan, places, n_rep),
        out_shape=tuple(jax.ShapeDtypeStruct(shape, BF16) for shape in outs)
        + (jax.ShapeDtypeStruct((2,) + small.shape, F32),),
        in_specs=[any_space] * len(flat) + [vmem],
        out_specs=(any_space,) * len(outs) + (vmem,),
        scratch_shapes=[
            pltpu.VMEM((base, width), BF16),
            pltpu.VMEM((base, width), BF16),
            pltpu.VMEM((box, width), BF16),
            pltpu.VMEM((2, width, unit), BF16),
            pltpu.VMEM((2 * bits + 2,) + small.shape, F32),
            pltpu.SemaphoreType.DMA((len(flat),)),
            pltpu.SemaphoreType.DMA((len(plan) + len(outs),)),
            pltpu.SemaphoreType.DMA((n_copies,)),
            pltpu.SemaphoreType.DMA((n_copies,)),
            pltpu.SemaphoreType.DMA((bits + 1,)),
            pltpu.SemaphoreType.DMA((bits + 1,)),
        ],
        compiler_params=pltpu.CompilerParams(
            collective_id=0, has_side_effects=True, vmem_limit_bytes=60 * 1024 * 1024
        ),
    )(*flat, small)
    return pieces, sums


def ffn_kernel(n2, cot, gate, up, down, hid_out, gg_out, ug_out, ng_out, ngb_out, dp_out, ng_acc, dp_acc):
    step = pl.program_id(0)

    @pl.when(step == 0)
    def _():
        ng_acc[...] = jnp.zeros_like(ng_acc)
        dp_acc[...] = jnp.zeros_like(dp_acc)

    gate_pre = mm_nt(gate[...], n2[...])
    up_proj = mm_nt(up[...], n2[...])
    hidden_grad = mm_nt(down[...], cot[...])
    sigmoid = 1.0 / (1.0 + jnp.exp(-gate_pre))
    activated = gate_pre * sigmoid
    hidden = (activated * up_proj).astype(BF16)
    gate_grad = (hidden_grad * up_proj * sigmoid * (1.0 + gate_pre * (1.0 - sigmoid))).astype(BF16)
    up_grad = (hidden_grad * activated).astype(BF16)
    hid_out[...] = hidden
    gg_out[...] = gate_grad
    ug_out[...] = up_grad
    ng_acc[...] += mm_tn(gate_grad, gate[...]) + mm_tn(up_grad, up[...])
    dp_acc[...] += mm_tn(hidden, down[...])

    @pl.when(step == pl.num_programs(0) - 1)
    def _():
        ng_out[...] = ng_acc[...]
        ngb_out[...] = ng_acc[...].astype(BF16)
        dp_out[...] = dp_acc[...].astype(dp_out.dtype)


def block_of(count, limit, grain):
    return max(d for d in range(grain, limit + 1, grain) if count % d == 0)


def ffn(n2, cot, gate, up, down, part_type):
    rows, width = n2.shape
    units = gate.shape[0]
    block = block_of(units, 512, 16)
    whole = pl.BlockSpec((rows, width), lambda i: (0, 0))
    cut = pl.BlockSpec((block, width), lambda i: (i, 0))
    cut_rows = pl.BlockSpec((block, rows), lambda i: (i, 0))
    wide = jax.ShapeDtypeStruct((units, rows), BF16)
    return pl.pallas_call(
        ffn_kernel,
        grid=(units // block,),
        out_shape=(
            wide,
            wide,
            wide,
            jax.ShapeDtypeStruct((rows, width), F32),
            jax.ShapeDtypeStruct((rows, width), BF16),
            jax.ShapeDtypeStruct((rows, width), part_type),
        ),
        in_specs=[whole, whole, cut, cut, cut],
        out_specs=(cut_rows, cut_rows, cut_rows, whole, whole, whole),
        scratch_shapes=[pltpu.VMEM((rows, width), F32), pltpu.VMEM((rows, width), F32)],
        compiler_params=pltpu.CompilerParams(vmem_limit_bytes=56 * 1024 * 1024),
        cost_estimate=pl.CostEstimate(
            flops=12 * units * rows * width, bytes_accessed=12 * units * width, transcendentals=units * rows
        ),
    )(n2, cot, gate, up, down)


def grads_kernel(hid_a, gg_a, ug_a, hid_b, gg_b, ug_b, n2_a, n2_b, cot_a, cot_b, dw, gw, uw):
    dw[...] = (mm_nn(hid_a[...], cot_a[...]) + mm_nn(hid_b[...], cot_b[...])).astype(BF16)
    gw[...] = (mm_nn(gg_a[...], n2_a[...]) + mm_nn(gg_b[...], n2_b[...])).astype(BF16)
    uw[...] = (mm_nn(ug_a[...], n2_a[...]) + mm_nn(ug_b[...], n2_b[...])).astype(BF16)


def ffn_grads(first, second, n2, cot):
    units, rows = first[0].shape
    width = n2[0].shape[1]
    block = block_of(units, 512, 16)
    whole = pl.BlockSpec((rows, width), lambda i: (0, 0))
    cut = pl.BlockSpec((block, width), lambda i: (i, 0))
    cut_rows = pl.BlockSpec((block, rows), lambda i: (i, 0))
    return pl.pallas_call(
        grads_kernel,
        grid=(units // block,),
        out_shape=(jax.ShapeDtypeStruct((units, width), BF16),) * 3,
        in_specs=[cut_rows] * 6 + [whole] * 4,
        out_specs=(cut,) * 3,
        compiler_params=pltpu.CompilerParams(vmem_limit_bytes=56 * 1024 * 1024),
        cost_estimate=pl.CostEstimate(
            flops=12 * units * rows * width, bytes_accessed=18 * units * width, transcendentals=0
        ),
    )(*first, *second, *n2, *cot)


def turn(x):
    return pltpu.roll(x, HEAD_SIZE // 2, 1)


def head_at(h):
    return pl.ds(pl.multiple_of(h * HEAD_SIZE, HEAD_SIZE), HEAD_SIZE)


def masked_scores(query, key, first, row, count, limit):
    scores = mm_nt(query, key) * (1.0 / math.sqrt(HEAD_SIZE))
    at = lax.broadcasted_iota(jnp.int32, (count, limit), 1)
    line = lax.broadcasted_iota(jnp.int32, (count, limit), 0) + row
    return jnp.where((at <= line) & (at >= first), scores, -1e30)


def front_kernel(
    tokens, gain, qw, kw, vw, qb, kb, vb, cos, sin, first, normed, queries, keys, values, mixed, logs
):
    rows = tokens.shape[0]
    heads = qw.shape[0] // HEAD_SIZE
    block = math.gcd(rows, 256)
    inputs = tokens[...].astype(F32)
    normed[...] = (inputs * rms_scale(inputs) * gain[...]).astype(BF16)
    keys_pre = mm_nt(normed[...], kw[...]) + kb[...]
    keys[...] = (keys_pre * cos[...] + turn(keys_pre) * sin[...]).astype(BF16)
    values[...] = (mm_nt(normed[...], vw[...]) + vb[...]).astype(BF16)
    logs[...] = jnp.zeros_like(logs)
    lane = lax.broadcasted_iota(jnp.int32, (block, HEAD_SIZE), 1)

    def one_head(h, carry):
        lanes = head_at(h)
        pre = mm_nt(normed[...], qw[lanes, :]) + qb[:, lanes]
        queries[:, lanes] = (pre * cos[...] + turn(pre) * sin[...]).astype(BF16)
        for row in range(0, rows, block):
            here, limit = pl.ds(row, block), row + block
            scores = masked_scores(queries[here, lanes], keys[:limit, :], first[here, :], row, block, limit)
            peak = jnp.max(scores, axis=1, keepdims=True)
            weights = jnp.exp(scores - peak)
            sums = jnp.sum(weights, axis=1, keepdims=True)
            logs[here, :] = jnp.where(lane == h, peak + jnp.log(sums), logs[here, :])
            probs = (weights * (1.0 / sums)).astype(BF16)
            mixed[here, lanes] = mm_nn(probs, values[:limit, :]).astype(BF16)
        return carry

    lax.fori_loop(0, heads, one_head, 0)


def front(tokens, gain, weights, biases, tables):
    rows, width = tokens.shape
    features = weights[0].shape[0]
    vmem = pl.BlockSpec(memory_space=pltpu.VMEM)
    return pl.pallas_call(
        front_kernel,
        out_shape=(
            jax.ShapeDtypeStruct((rows, width), BF16),
            jax.ShapeDtypeStruct((rows, features), BF16),
            jax.ShapeDtypeStruct((rows, HEAD_SIZE), BF16),
            jax.ShapeDtypeStruct((rows, HEAD_SIZE), BF16),
            jax.ShapeDtypeStruct((rows, features), BF16),
            jax.ShapeDtypeStruct((rows, HEAD_SIZE), F32),
        ),
        in_specs=[vmem] * 11,
        out_specs=(vmem,) * 6,
        compiler_params=pltpu.CompilerParams(vmem_limit_bytes=48 * 1024 * 1024),
        cost_estimate=pl.CostEstimate(
            flops=40 * rows * features * (width + rows), bytes_accessed=80 * rows * width, transcendentals=0
        ),
    )(tokens, gain, *weights, *biases, *tables)


def project_kernel(mixed, ow, part, part_b):
    part[...] = mm_nt(mixed[...], ow[...])
    part_b[...] = part[...].astype(BF16)


def project(mixed, output_cols):
    shape = mixed.shape[0], output_cols.shape[0]
    vmem = pl.BlockSpec(memory_space=pltpu.VMEM)
    return pl.pallas_call(
        project_kernel,
        out_shape=(jax.ShapeDtypeStruct(shape, F32), jax.ShapeDtypeStruct(shape, BF16)),
        in_specs=[vmem] * 2,
        out_specs=(vmem,) * 2,
        compiler_params=pltpu.CompilerParams(vmem_limit_bytes=16 * 1024 * 1024),
        cost_estimate=pl.CostEstimate(
            flops=2 * mixed.size * shape[1], bytes_accessed=16 * mixed.size, transcendentals=0
        ),
    )(mixed, output_cols)


def back_kernel(
    grad, ow, mixed, queries, keys, values, logs, cos, sin, first, qw, kw, vw, joined, sums, out, out_b, mg, dk, dv
):
    rows, features = queries.shape
    heads = features // HEAD_SIZE
    block = math.gcd(rows, 256)
    scale = 1.0 / math.sqrt(HEAD_SIZE)
    mg[...] = mm_nn(grad[...], ow[...]).astype(BF16)
    dk[...] = jnp.zeros_like(dk)
    dv[...] = jnp.zeros_like(dv)
    lane = lax.broadcasted_iota(jnp.int32, (block, HEAD_SIZE), 1)

    def one_head(h, carry):
        lanes = head_at(h)
        total = jnp.zeros((1, HEAD_SIZE), F32)
        for row in range(0, rows, block):
            here, limit = pl.ds(row, block), row + block
            query, grads = queries[here, lanes], mg[here, lanes]
            scores = masked_scores(query, keys[:limit, :], first[here, :], row, block, limit)
            log_total = jnp.sum(jnp.where(lane == h, logs[here, :], 0.0), axis=1, keepdims=True)
            probs = jnp.exp(scores - log_total)
            delta = jnp.sum(grads.astype(F32) * mixed[here, lanes].astype(F32), axis=1, keepdims=True)
            probs_grad = mm_nt(grads, values[:limit, :])
            score_grad = (probs * (probs_grad - delta) * scale).astype(BF16)
            dv[:limit, :] += mm_tn(probs.astype(BF16), grads)
            dk[:limit, :] += mm_tn(score_grad, query)
            dq = mm_nn(score_grad, keys[:limit, :])
            dq = dq * cos[here, :] - turn(dq) * sin[here, :]
            total = total + jnp.sum(dq, axis=0, keepdims=True)
            joined[here, lanes] = dq.astype(BF16)
        sums[:, lanes] = total
        return carry

    lax.fori_loop(0, heads, one_head, 0)
    keys_grad = dk[...] * cos[...] - turn(dk[...]) * sin[...]
    for k, piece in enumerate((keys_grad, dv[...])):
        lanes = pl.ds(features + k * HEAD_SIZE, HEAD_SIZE)
        sums[:, lanes] = jnp.sum(piece, axis=0, keepdims=True)
        joined[:, lanes] = piece.astype(BF16)
    out[...] = (
        mm_nn(joined[:, :features], qw[...])
        + mm_nn(joined[:, features : features + HEAD_SIZE], kw[...])
        + mm_nn(joined[:, features + HEAD_SIZE :], vw[...])
    )
    out_b[...] = out[...].astype(BF16)


def back(grad, output_cols, kept, tables, weights):
    rows, width = grad.shape
    features = weights[0].shape[0]
    vmem = pl.BlockSpec(memory_space=pltpu.VMEM)
    return pl.pallas_call(
        back_kernel,
        out_shape=(
            jax.ShapeDtypeStruct((rows, features + 2 * HEAD_SIZE), BF16),
            jax.ShapeDtypeStruct((1, features + 2 * HEAD_SIZE), F32),
            jax.ShapeDtypeStruct((rows, width), F32),
            jax.ShapeDtypeStruct((rows, width), BF16),
        ),
        in_specs=[vmem] * 13,
        out_specs=(vmem,) * 4,
        scratch_shapes=[
            pltpu.VMEM((rows, features), BF16),
            pltpu.VMEM((rows, HEAD_SIZE), F32),
            pltpu.VMEM((rows, HEAD_SIZE), F32),
        ],
        compiler_params=pltpu.CompilerParams(vmem_limit_bytes=48 * 1024 * 1024),
        cost_estimate=pl.CostEstimate(
            flops=40 * rows * features * (width + 2 * rows), bytes_accessed=80 * rows * width, transcendentals=0
        ),
    )(grad, output_cols, *kept, *tables, *weights)


def mask_and_tables(lengths, rows):
    ends = jnp.cumsum(lengths)
    starts = ends - lengths
    row = jnp.arange(rows, dtype=jnp.int32)
    inside = (row[:, None] >= starts[None, :]) & (row[:, None] < ends[None, :])
    first = jnp.sum(jnp.where(inside, starts[None, :], 0), axis=1)
    cosine, sine = rotary_tables(row - first, HEAD_SIZE)
    half = HEAD_SIZE // 2
    sine = jnp.concatenate([-sine[:, :half], sine[:, half:]], axis=1)
    return cosine, sine, first[:, None]


def local(
    n_rep,
    tokens,
    query_weight,
    key_weight,
    value_weight,
    query_bias,
    key_bias,
    value_bias,
    output_matrix,
    gate_weight,
    up_weight,
    down_weight,
    attn_gain,
    mlp_gain,
    cotangent,
    seq_lengths,
):
    g = lax.axis_index("grp")
    rows = tokens.shape[0]

    gains = jnp.stack([attn_gain, mlp_gain])
    gains_other = swap(gains)
    tokens_other = swap(tokens)
    lengths_other = swap(seq_lengths)
    cut = output_matrix.shape[1] // 2
    given = jnp.concatenate([half_of(output_matrix, 1 - g, 1), half_of(down_weight, 1 - g, 1)], axis=1)
    shared = swap_shared(given, n_rep)
    gains = in_order(gains, gains_other, g, 1).astype(F32)
    attn_gain_all, mlp_gain_all = gains[0:1], gains[1:2]
    output_cols = in_order(half_of(output_matrix, g, 1), shared[:, :cut], g)
    down_rows = in_order(half_of(down_weight, g, 1), shared[:, cut:], g).T

    weights = (query_weight, key_weight, value_weight)
    biases = tuple(b.astype(F32)[None, :] for b in (query_bias, key_bias, value_bias))

    def begin(token_rows, lengths):
        tables = mask_and_tables(lengths[0], rows)
        normed, queries, keys, values, mixed, logs = front(token_rows, attn_gain_all, weights, biases, tables)
        inputs = token_rows.astype(F32)
        return dict(
            inputs=inputs,
            unit=inputs * rms_scale(inputs),
            scale=rms_scale(inputs),
            normed=normed,
            kept=(mixed, queries, keys, values, logs),
            tables=tables,
        )

    own = begin(tokens, seq_lengths)
    cotangent_other = swap(after(cotangent, own["kept"][0]))
    own["part"], part_own_b = project(own["kept"][0], output_cols)
    came_other = swap(part_own_b)
    oth = begin(after(tokens_other, own["kept"][0]), lengths_other)
    oth["part"], part_oth_b = project(oth["kept"][0], output_cols)
    came_own = swap(after(part_oth_b, part_own_b))

    def middle(kept, came, cot, part_type):
        residual = kept["inputs"] + kept["part"] + came.astype(F32)
        scale = rms_scale(residual)
        normed = (residual * scale * mlp_gain_all).astype(BF16)
        *wide, grad, grad_b, part = ffn(normed, cot, gate_weight, up_weight, down_rows, part_type)
        return dict(residual=residual, scale=scale, normed=normed, wide=wide, grad=grad, grad_b=grad_b, part=part)

    mid_oth = middle(oth, came_other, cotangent_other, BF16)
    grad_came_own = swap(mid_oth["grad_b"])
    mid_own = middle(own, came_own, cotangent, F32)
    grad_came_oth = swap(after(mid_own["grad_b"], grad_came_own))
    down_came = swap(after(mid_oth["part"], grad_came_oth))
    block_out = mid_own["residual"] + mid_own["part"] + down_came.astype(F32)
    down_grad, gate_weight_grad, up_weight_grad = ffn_grads(
        mid_oth["wide"],
        mid_own["wide"],
        (mid_oth["normed"], mid_own["normed"]),
        (cotangent_other, cotangent),
    )

    def middle_grad(mid, came, cot):
        normed_grad = mid["grad"] + came.astype(F32)
        unit = mid["residual"] * mid["scale"]
        gain_grad = jnp.sum(normed_grad * unit, axis=0)
        unit_grad = normed_grad * mlp_gain_all
        residual_grad = cot.astype(F32) + mid["scale"] * (
            unit_grad - unit * jnp.mean(unit_grad * unit, axis=-1, keepdims=True)
        )
        return residual_grad, residual_grad.astype(BF16), gain_grad

    residual_grad_own, residual_grad_own_b, gain_grad_own = middle_grad(mid_own, grad_came_own, cotangent)
    _, residual_grad_oth_b, gain_grad_oth = middle_grad(mid_oth, grad_came_oth, cotangent_other)
    mlp_gain_grad = gain_grad_own + gain_grad_oth

    joined_own, sums_own, front_own, _ = back(residual_grad_own_b, output_cols, own["kept"], own["tables"], weights)
    joined_oth, sums_oth, front_oth, front_oth_b = back(
        residual_grad_oth_b, output_cols, oth["kept"], oth["tables"], weights
    )
    front_came = swap(after(front_oth_b, down_came))
    output_grad = mm_tn(
        jnp.concatenate([own["kept"][0], oth["kept"][0]]), jnp.concatenate([residual_grad_own_b, residual_grad_oth_b])
    ).astype(BF16)
    projections = mm_tn(
        jnp.concatenate([joined_own, joined_oth]), jnp.concatenate([own["normed"], oth["normed"]])
    ).astype(BF16)
    attn_gain_grad = jnp.sum(front_own * own["unit"] + front_oth * oth["unit"], axis=0)
    front_own = front_own + front_came.astype(F32)
    unit_grad = front_own * attn_gain_all
    input_grad = residual_grad_own + own["scale"] * (
        unit_grad - own["unit"] * jnp.mean(unit_grad * own["unit"], axis=-1, keepdims=True)
    )

    small = jnp.concatenate([(sums_own + sums_oth)[0], half_of(mlp_gain_grad, g, 0), attn_gain_grad])
    count = small.shape[0]
    lines = -(-count // (8 * 128)) * 8
    small = jnp.pad(small, (0, lines * 128 - count)).reshape(lines, 128)
    units, features = gate_weight.shape[0], query_weight.shape[0]
    pieces, small = sum_pool(
        [
            ([down_grad], [units], True),
            ([gate_weight_grad, up_weight_grad], [units, units], False),
            ([output_grad], [features], True),
            ([projections], [w.shape[0] for w in weights], False),
        ],
        small,
        n_rep,
    )
    small = small.reshape(2, -1)
    vectors, at = [], 0
    for piece in (query_bias, key_bias, value_bias, mlp_gain):
        vectors.append(small[0, at : at + piece.shape[0]])
        at += piece.shape[0]
    vectors.append(half_of(small[0, at:count] + small[1, at:count], g, 0))
    half = down_grad.shape[1] // 2

    def owned(piece, count):
        return jnp.concatenate([piece[:half, :count], piece[half:, :count]], axis=1).astype(F32)

    return (
        block_out,
        input_grad,
        pieces[4].astype(F32),
        pieces[5].astype(F32),
        pieces[6].astype(F32),
        vectors[0],
        vectors[1],
        vectors[2],
        owned(pieces[3], features),
        pieces[1].astype(F32),
        pieces[2].astype(F32),
        owned(pieces[0], units),
        vectors[4],
        vectors[3],
    )


def solution(mesh):
    n_rep = mesh.shape["rep"]
    assert mesh.shape["grp"] == 2 and n_rep & (n_rep - 1) == 0
    rows = P(("rep", "grp"), None)
    wide, flat = P("grp", None), P("grp")

    def body(*args):
        return local(n_rep, *args)

    return jax.shard_map(
        body,
        mesh=mesh,
        in_specs=(rows, wide, wide, wide, flat, flat, flat, wide, wide, wide, wide, flat, flat, rows, rows),
        out_specs=(rows, rows, wide, wide, wide, flat, flat, flat, wide, wide, wide, wide, flat, flat),
        check_vma=False,
    )
```

```python
import functools
import math

import jax
import jax.numpy as jnp
from jax import lax
from jax.experimental import pallas as pl
from jax.experimental.pallas import tpu as pltpu
from jax.sharding import PartitionSpec as P


HEAD_SIZE = 128

EPSILON = 1e-06
THETA = 1000000.0

BF16 = jnp.bfloat16
F32 = jnp.float32
MESH = pl.DeviceIdType.MESH


def mm_nt(left, right):
    return lax.dot_general(left, right, (((1,), (1,)), ((), ())), preferred_element_type=F32)


def mm_nn(left, right):
    return lax.dot_general(left, right, (((1,), (0,)), ((), ())), preferred_element_type=F32)


def mm_tn(left, right):
    return lax.dot_general(left, right, (((0,), (0,)), ((), ())), preferred_element_type=F32)


def rotary_tables(position, head_dim):
    half_dim = head_dim // 2
    exponent = jnp.arange(half_dim, dtype=F32) * (2.0 / head_dim)
    frequency = jnp.exp(-exponent * math.log(THETA))
    angles = position.astype(F32)[:, None] * frequency[None, :]
    cosine = jnp.cos(angles)
    sine = jnp.sin(angles)
    return (jnp.concatenate([cosine, cosine], axis=-1), jnp.concatenate([sine, sine], axis=-1))


def rms_scale(values):
    return lax.rsqrt(jnp.mean(values * values, axis=-1, keepdims=True) + EPSILON)


def swap(x):
    return lax.ppermute(x, "grp", [(0, 1), (1, 0)])


def after(x, earlier):
    return lax.optimization_barrier((x, earlier))[0]


def swap_shared(x, n_rep, levels=2):
    levels = min(levels, n_rep.bit_length() - 1)
    me = lax.axis_index("rep")
    count = x.shape[0] >> levels
    came = piece = swap(lax.dynamic_slice_in_dim(x, (me & ((1 << levels) - 1)) * count, count, 0))
    for b in range(levels):
        shared = lax.ppermute(came, "rep", [(i, i ^ (1 << b)) for i in range(n_rep)])
        came = in_order(came, shared, (me >> b) & 1)
    return came, piece


def in_order(mine, other, g, axis=0):
    first = jnp.where(g == 0, mine, other)
    second = jnp.where(g == 0, other, mine)
    return jnp.concatenate([first, second], axis)


def half_of(x, which, axis):
    size = x.shape[axis] // 2
    return lax.dynamic_slice_in_dim(x, which * size, size, axis)


def rows_loop(count, step, body):
    def one(i, carry):
        body(pl.multiple_of(i * step, step), step)
        return carry

    lax.fori_loop(0, count // step, one, 0)


def pool_kernel(plan, groups, n_factors, slots, n_rep, *refs):
    n_parts = sum(2 if made else len(parts) for _, parts, _, _, _, made in groups)
    n_outs = sum(1 if cross else len(cuts) for _, _, _, cuts, cross, _ in groups)
    ins, factors, refs = refs[:n_parts], refs[n_parts : n_parts + n_factors], refs[n_parts + n_factors :]
    small_ref, refs = refs[0], refs[1:]
    outs, small_out, refs = refs[:n_outs], refs[n_outs], refs[n_outs + 1 :]
    pool, full, inbox, flipped, lefts, small_box, in_sem, left_sem, out_sem, *refs = refs
    send_sem, recv_sem, small_send, small_recv = refs
    me, g = lax.axis_index("rep"), lax.axis_index("grp")
    bits = n_rep.bit_length() - 1
    half = pool.shape[1] // 2

    barrier = pltpu.get_barrier_semaphore()
    for b in range(bits):
        pl.semaphore_signal(barrier, inc=1, device_id={"rep": me ^ (1 << b)}, device_id_type=MESH)
    pl.semaphore_signal(barrier, inc=1, device_id={"grp": 1 - g}, device_id_type=MESH)

    loads, at = [], 0
    makers = {}
    for k, (base, parts, end, _, _, made) in enumerate(groups):
        loads.append([])
        if made:
            makers[k] = ins[at : at + 2], [factors[f] for f in made]
            at, base = at + 2, base + parts[0]
        else:
            for count in parts:
                loads[-1].append(pltpu.make_async_copy(ins[at], pool.at[pl.ds(base, count)], in_sem.at[at]))
                loads[-1][-1].start()
                base, at = base + count, at + 1
        if base < end:
            pool[pl.ds(base, end - base), :] = jnp.zeros((end - base, pool.shape[1]), BF16)
    made_units = [u for u, unit in enumerate(plan) if unit[3] in makers]
    fetched = {}

    def fetch(k):
        if k < len(made_units):
            u = made_units[k]
            start, size, _, group, _ = plan[u]
            base, parts = groups[group][:2]
            count = min(size, base + parts[0] - start)
            fetched[u] = count, []
            for side, source in enumerate(makers[group][0]):
                copy = pltpu.make_async_copy(
                    source.at[pl.ds(start - base, count)], lefts.at[k % slots, side, pl.ds(0, count)], left_sem.at[k, side]
                )
                copy.start()
                fetched[u][1].append(copy)

    def make(u):
        k = made_units.index(u)
        start, _, _, group, _ = plan[u]
        count, waits = fetched[u]
        for copy in waits:
            copy.wait()
        first, second = makers[group][1]
        product = mm_nn(lefts[k % slots, 0, :count, :], first[...]) + mm_nn(lefts[k % slots, 1, :count, :], second[...])
        pool[pl.ds(start, count), :] = product.astype(BF16)
        fetch(k + slots)

    for k in range(slots):
        fetch(k)
    small_box[0] = small_ref[...]
    pl.semaphore_wait(barrier, bits + 1)

    copies, state, box_at, used = {}, {}, {}, 0
    for u, (start, size, order, group, cross) in enumerate(plan):
        n = size
        for s in range(bits):
            n //= 2
            box_at[u, s] = used
            used += n
    loaded, numbers, leaving, flips, count_of_flips = set(), {}, [], [], [0]

    def remote(source, target, key, there):
        at = numbers.setdefault(key, len(numbers))
        copies[key] = pltpu.make_async_remote_copy(
            src_ref=source,
            dst_ref=target,
            send_sem=send_sem.at[at],
            recv_sem=recv_sem.at[at],
            device_id=there,
            device_id_type=MESH,
        )
        copies[key].start()

    def bit_of(b):
        return (me >> b) & 1

    def advance(u, step):
        start, size, order, group, cross = plan[u]
        kinds = ["halve"] * bits + ["cross"] * cross + ["double"] * bits + ["out"]
        if step == 0:
            if group not in loaded:
                loaded.add(group)
                for load in loads[group]:
                    load.wait()
            if group in makers:
                make(u)
            state[u] = [jnp.int32(start), size]
        else:
            copies[u, step - 1].wait()
            before = kinds[step - 1]
            off, n = state[u]
            if before == "halve":
                n //= 2
                at = box_at[u, step - 1]
                keep = pl.multiple_of(off + bit_of(order[step - 1]) * n, n)
                target = full if kinds[step] == "double" else pool

                def add(i, count):
                    there = pl.ds(pl.multiple_of(keep + i, 16), count)
                    here = pl.ds(pl.multiple_of(at + i, 16), count)
                    target[there, :] = (pool[there, :].astype(F32) + inbox[here, :].astype(F32)).astype(BF16)

                rows_loop(n, 16 if n % 32 else 32, add)
                state[u] = [keep, n]
            elif before == "double":
                b = order[2 * bits + cross - step]
                state[u] = [pl.multiple_of(off - bit_of(b) * n, n), 2 * n]
        off, n = state[u]
        kind = kinds[step]
        if kind == "halve":
            n //= 2
            b = order[step]
            give = pl.multiple_of(off + (1 - bit_of(b)) * n, n)
            target = inbox.at[pl.ds(box_at[u, step], n)]
            remote(pool.at[pl.ds(give, n)], target, (u, step), {"rep": me ^ (1 << b)})
        elif kind == "cross":
            rows = pl.ds(off, n)
            mine = pl.ds(pl.multiple_of(g * half, 128), half)
            theirs = pl.ds(pl.multiple_of((1 - g) * half, 128), half)
            remote(pool.at[rows, theirs], full.at[rows, mine], (u, step), {"grp": 1 - g})
            full[rows, mine] = pool[rows, mine]
        elif kind == "double":
            b = order[2 * bits + cross - 1 - step]
            block = pl.ds(off, n)
            remote(full.at[block], full.at[block], (u, step), {"rep": me ^ (1 << b)})
        else:
            first = sum(1 if c else len(cuts) for _, _, _, cuts, c, _ in groups[:group])
            base, cuts = groups[group][0], groups[group][3]
            wanted = []
            if cross:
                slot = count_of_flips[0] % slots
                if count_of_flips[0] >= slots:
                    flips[count_of_flips[0] - slots].wait()
                count_of_flips[0] += 1

                def flip(i, count):
                    piece = full[pl.ds(pl.multiple_of(start + i, 128), count), :].astype(F32)
                    flipped[slot, :, pl.ds(pl.multiple_of(i, 128), count)] = piece.T.astype(BF16)

                rows_loop(size, 128, flip)
                wanted.append((flipped.at[slot, :, pl.ds(0, size)], outs[first].at[:, pl.ds(start - base, size)]))
            for k, count in enumerate(() if cross else cuts):
                low, high = max(base, start), min(base + count, start + size)
                if low < high:
                    wanted.append((full.at[pl.ds(low, high - low)], outs[first + k].at[pl.ds(low - base, high - low)]))
                base += count
            for source, target in wanted:
                copy = pltpu.make_async_copy(source, target, out_sem.at[len(leaving) + len(flips)])
                copy.start()
                (flips if cross else leaving).append(copy)

    def advance_small(s):
        if s > 0:
            copies["small", s - 1].wait()
            if s <= bits:
                small_box[2 * s] = small_box[2 * s - 2] + small_box[2 * s - 1]
        if s <= bits:
            copies["small", s] = pltpu.make_async_remote_copy(
                src_ref=small_box.at[2 * s],
                dst_ref=small_box.at[2 * s + 1],
                send_sem=small_send.at[s],
                recv_sem=small_recv.at[s],
                device_id={"rep": me ^ (1 << s)} if s < bits else {"grp": 1 - g},
                device_id_type=MESH,
            )
            copies["small", s].start()
        else:
            small_out[0] = small_box[2 * bits]
            small_out[1] = small_box[2 * bits + 1]

    steps = [2 * bits + 1 + cross for *_, cross in plan]
    for t in range(max(u + n for u, n in enumerate(steps))):
        for u in range(len(plan)):
            if 0 <= t - u < steps[u]:
                advance(u, t - u)
        if t <= bits + 1:
            advance_small(t)
    for copy in leaving + flips[-slots:]:
        copy.wait()


def sum_pool(groups, factors, small, n_rep):
    bits = n_rep.bit_length() - 1
    straight = tuple(range(bits))
    grain = 16 * n_rep
    unit = max(768 // grain, 1) * grain
    flat = [a for arrays, *_ in groups for a in arrays]
    width = factors[0].shape[1]
    slots = 2 if n_rep <= 16 else 1
    plan, places, outs, base = [], [], [], 0
    for k, (arrays, cuts, cross, made) in enumerate(groups):
        counts = [a.shape[0] for a in arrays[: 1 if made else None]]
        end = base + -(-sum(counts) // grain) * grain
        places.append((base, counts, end, cuts, cross, made))
        for start in range(base, end, unit):
            plan.append((start, min(unit, end - start), straight, k, int(cross)))
        outs += [(width, end - base)] if cross else [(count, width) for count in cuts]
        base = end
    box = sum(size - size // n_rep for _, size, *_ in plan)
    n_copies = sum(2 * bits + cross for *_, cross in plan)
    any_space = pl.BlockSpec(memory_space=pl.ANY)
    vmem = pl.BlockSpec(memory_space=pltpu.VMEM)
    *pieces, sums = pl.pallas_call(
        functools.partial(pool_kernel, plan, places, len(factors), slots, n_rep),
        out_shape=tuple(jax.ShapeDtypeStruct(shape, BF16) for shape in outs)
        + (jax.ShapeDtypeStruct((2,) + small.shape, F32),),
        in_specs=[any_space] * len(flat) + [vmem] * (len(factors) + 1),
        out_specs=(any_space,) * len(outs) + (vmem,),
        scratch_shapes=[
            pltpu.VMEM((base, width), BF16),
            pltpu.VMEM((base, width), BF16),
            pltpu.VMEM((box, width), BF16),
            pltpu.VMEM((slots, width, unit), BF16),
            pltpu.VMEM((slots, 2, unit, factors[0].shape[0]), BF16),
            pltpu.VMEM((2 * bits + 2,) + small.shape, F32),
            pltpu.SemaphoreType.DMA((len(flat),)),
            pltpu.SemaphoreType.DMA((len(plan), 2)),
            pltpu.SemaphoreType.DMA((len(plan) + len(outs),)),
            pltpu.SemaphoreType.DMA((n_copies,)),
            pltpu.SemaphoreType.DMA((n_copies,)),
            pltpu.SemaphoreType.DMA((bits + 1,)),
            pltpu.SemaphoreType.DMA((bits + 1,)),
        ],
        compiler_params=pltpu.CompilerParams(
            collective_id=0, has_side_effects=True, vmem_limit_bytes=62 * 1024 * 1024
        ),
    )(*flat, *factors, small)
    return pieces, sums


def ffn_kernel(
    tokens, part, came, gain, cot, gate, up, down, residual, n2, hid_out, gg_out, ug_out, ng_out, ngb_out, dp_out, ng_acc, dp_acc
):
    step = pl.program_id(0)

    @pl.when(step == 0)
    def _():
        total = tokens[...].astype(F32) + part[...] + came[...].astype(F32)
        residual[...] = total
        n2[...] = (total * rms_scale(total) * gain[...]).astype(BF16)
        ng_acc[...] = jnp.zeros_like(ng_acc)
        dp_acc[...] = jnp.zeros_like(dp_acc)

    gate_pre = mm_nt(gate[...], n2[...])
    up_proj = mm_nt(up[...], n2[...])
    hidden_grad = mm_nt(down[...], cot[...])
    sigmoid = 1.0 / (1.0 + jnp.exp(-gate_pre))
    activated = gate_pre * sigmoid
    hidden = (activated * up_proj).astype(BF16)
    gate_grad = (hidden_grad * up_proj * sigmoid * (1.0 + gate_pre * (1.0 - sigmoid))).astype(BF16)
    up_grad = (hidden_grad * activated).astype(BF16)
    hid_out[...] = hidden
    gg_out[...] = gate_grad
    ug_out[...] = up_grad
    ng_acc[...] += mm_tn(gate_grad, gate[...]) + mm_tn(up_grad, up[...])
    dp_acc[...] += mm_tn(hidden, down[...])

    @pl.when(step == pl.num_programs(0) - 1)
    def _():
        ng_out[...] = ng_acc[...]
        ngb_out[...] = ng_acc[...].astype(BF16)
        dp_out[...] = dp_acc[...].astype(dp_out.dtype)


def block_of(count, limit, grain):
    return max(d for d in range(grain, limit + 1, grain) if count % d == 0)


def ffn(tokens, part, came, gain, cot, gate, up, down, part_type):
    rows, width = tokens.shape
    units = gate.shape[0]
    block = block_of(units, 512, 16)
    whole = pl.BlockSpec((rows, width), lambda i: (0, 0))
    cut = pl.BlockSpec((block, width), lambda i: (i, 0))
    cut_rows = pl.BlockSpec((block, rows), lambda i: (i, 0))
    wide = jax.ShapeDtypeStruct((units, rows), BF16)
    return pl.pallas_call(
        ffn_kernel,
        grid=(units // block,),
        out_shape=(
            jax.ShapeDtypeStruct((rows, width), F32),
            jax.ShapeDtypeStruct((rows, width), BF16),
            wide,
            wide,
            wide,
            jax.ShapeDtypeStruct((rows, width), F32),
            jax.ShapeDtypeStruct((rows, width), BF16),
            jax.ShapeDtypeStruct((rows, width), part_type),
        ),
        in_specs=[whole, whole, whole, pl.BlockSpec((1, width), lambda i: (0, 0)), whole, cut, cut, cut],
        out_specs=(whole, whole, cut_rows, cut_rows, cut_rows, whole, whole, whole),
        scratch_shapes=[pltpu.VMEM((rows, width), F32), pltpu.VMEM((rows, width), F32)],
        compiler_params=pltpu.CompilerParams(vmem_limit_bytes=56 * 1024 * 1024),
        cost_estimate=pl.CostEstimate(
            flops=12 * units * rows * width, bytes_accessed=12 * units * width, transcendentals=units * rows
        ),
    )(tokens, part, came, gain, cot, gate, up, down)


def turn(x):
    return pltpu.roll(x, HEAD_SIZE // 2, 1)


def head_at(h):
    return pl.ds(pl.multiple_of(h * HEAD_SIZE, HEAD_SIZE), HEAD_SIZE)


def masked_scores(query, key, first, row, count, limit):
    scores = mm_nt(query, key) * (1.0 / math.sqrt(HEAD_SIZE))
    at = lax.broadcasted_iota(jnp.int32, (count, limit), 1)
    line = lax.broadcasted_iota(jnp.int32, (count, limit), 0) + row
    return jnp.where((at <= line) & (at >= first), scores, -1e30)


def front_kernel(
    tokens, gain, qw, kw, vw, qb, kb, vb, cos, sin, first, normed, queries, keys, values, mixed, logs
):
    rows = tokens.shape[0]
    heads = qw.shape[0] // HEAD_SIZE
    block = math.gcd(rows, 256)
    inputs = tokens[...].astype(F32)
    normed[...] = (inputs * rms_scale(inputs) * gain[...]).astype(BF16)
    keys_pre = mm_nt(normed[...], kw[...]) + kb[...]
    keys[...] = (keys_pre * cos[...] + turn(keys_pre) * sin[...]).astype(BF16)
    values[...] = (mm_nt(normed[...], vw[...]) + vb[...]).astype(BF16)
    logs[...] = jnp.zeros_like(logs)
    lane = lax.broadcasted_iota(jnp.int32, (block, HEAD_SIZE), 1)

    def one_head(h, carry):
        lanes = head_at(h)
        pre = mm_nt(normed[...], qw[lanes, :]) + qb[:, lanes]
        queries[:, lanes] = (pre * cos[...] + turn(pre) * sin[...]).astype(BF16)
        for row in range(0, rows, block):
            here, limit = pl.ds(row, block), row + block
            scores = masked_scores(queries[here, lanes], keys[:limit, :], first[here, :], row, block, limit)
            peak = jnp.max(scores, axis=1, keepdims=True)
            weights = jnp.exp(scores - peak)
            sums = jnp.sum(weights, axis=1, keepdims=True)
            logs[here, :] = jnp.where(lane == h, peak + jnp.log(sums), logs[here, :])
            probs = (weights * (1.0 / sums)).astype(BF16)
            mixed[here, lanes] = mm_nn(probs, values[:limit, :]).astype(BF16)
        return carry

    lax.fori_loop(0, heads, one_head, 0)


def front(tokens, gain, weights, biases, tables):
    rows, width = tokens.shape
    features = weights[0].shape[0]
    vmem = pl.BlockSpec(memory_space=pltpu.VMEM)
    return pl.pallas_call(
        front_kernel,
        out_shape=(
            jax.ShapeDtypeStruct((rows, width), BF16),
            jax.ShapeDtypeStruct((rows, features), BF16),
            jax.ShapeDtypeStruct((rows, HEAD_SIZE), BF16),
            jax.ShapeDtypeStruct((rows, HEAD_SIZE), BF16),
            jax.ShapeDtypeStruct((rows, features), BF16),
            jax.ShapeDtypeStruct((rows, HEAD_SIZE), F32),
        ),
        in_specs=[vmem] * 11,
        out_specs=(vmem,) * 6,
        compiler_params=pltpu.CompilerParams(vmem_limit_bytes=48 * 1024 * 1024),
        cost_estimate=pl.CostEstimate(
            flops=40 * rows * features * (width + rows), bytes_accessed=80 * rows * width, transcendentals=0
        ),
    )(tokens, gain, *weights, *biases, *tables)


def project_kernel(mixed, ow, part, part_b):
    part[...] = mm_nt(mixed[...], ow[...])
    part_b[...] = part[...].astype(BF16)


def project(mixed, output_cols):
    shape = mixed.shape[0], output_cols.shape[0]
    vmem = pl.BlockSpec(memory_space=pltpu.VMEM)
    return pl.pallas_call(
        project_kernel,
        out_shape=(jax.ShapeDtypeStruct(shape, F32), jax.ShapeDtypeStruct(shape, BF16)),
        in_specs=[vmem] * 2,
        out_specs=(vmem,) * 2,
        compiler_params=pltpu.CompilerParams(vmem_limit_bytes=16 * 1024 * 1024),
        cost_estimate=pl.CostEstimate(
            flops=2 * mixed.size * shape[1], bytes_accessed=16 * mixed.size, transcendentals=0
        ),
    )(mixed, output_cols)


def back_kernel(
    tokens, grad, came, residual, cot, gain, ow, mixed, queries, keys, values, logs, cos, sin, first, qw, kw, vw,
    residual_grad, residual_grad_b, gain_grad, front_gain_grad, joined, sums, out, out_b, mg, dk, dv
):
    rows, features = queries.shape
    heads = features // HEAD_SIZE
    block = math.gcd(rows, 256)
    scale = 1.0 / math.sqrt(HEAD_SIZE)
    normed_grad = grad[...] + came[...].astype(F32)
    norm = rms_scale(residual[...])
    unit = residual[...] * norm
    gain_grad[...] = jnp.sum(normed_grad * unit, axis=0, keepdims=True)
    unit_grad = normed_grad * gain[...]
    along = jnp.mean(unit_grad * unit, axis=1, keepdims=True)
    residual_grad[...] = cot[...].astype(F32) + norm * (unit_grad - unit * along)
    residual_grad_b[...] = residual_grad[...].astype(BF16)
    mg[...] = mm_nn(residual_grad_b[...], ow[...]).astype(BF16)
    dk[...] = jnp.zeros_like(dk)
    dv[...] = jnp.zeros_like(dv)
    lane = lax.broadcasted_iota(jnp.int32, (block, HEAD_SIZE), 1)

    def one_head(h, carry):
        lanes = head_at(h)
        total = jnp.zeros((1, HEAD_SIZE), F32)
        for row in range(0, rows, block):
            here, limit = pl.ds(row, block), row + block
            query, grads = queries[here, lanes], mg[here, lanes]
            scores = masked_scores(query, keys[:limit, :], first[here, :], row, block, limit)
            log_total = jnp.sum(jnp.where(lane == h, logs[here, :], 0.0), axis=1, keepdims=True)
            probs = jnp.exp(scores - log_total)
            delta = jnp.sum(grads.astype(F32) * mixed[here, lanes].astype(F32), axis=1, keepdims=True)
            probs_grad = mm_nt(grads, values[:limit, :])
            score_grad = (probs * (probs_grad - delta) * scale).astype(BF16)
            dv[:limit, :] += mm_tn(probs.astype(BF16), grads)
            dk[:limit, :] += mm_tn(score_grad, query)
            dq = mm_nn(score_grad, keys[:limit, :])
            dq = dq * cos[here, :] - turn(dq) * sin[here, :]
            total = total + jnp.sum(dq, axis=0, keepdims=True)
            joined[here, lanes] = dq.astype(BF16)
        sums[:, lanes] = total
        return carry

    lax.fori_loop(0, heads, one_head, 0)
    keys_grad = dk[...] * cos[...] - turn(dk[...]) * sin[...]
    for k, piece in enumerate((keys_grad, dv[...])):
        lanes = pl.ds(features + k * HEAD_SIZE, HEAD_SIZE)
        sums[:, lanes] = jnp.sum(piece, axis=0, keepdims=True)
        joined[:, lanes] = piece.astype(BF16)
    out[...] = (
        mm_nn(joined[:, :features], qw[...])
        + mm_nn(joined[:, features : features + HEAD_SIZE], kw[...])
        + mm_nn(joined[:, features + HEAD_SIZE :], vw[...])
    )
    out_b[...] = out[...].astype(BF16)
    inputs = tokens[...].astype(F32)
    front_gain_grad[...] = jnp.sum(out[...] * (inputs * rms_scale(inputs)), axis=0, keepdims=True)


def back(tokens, grad, came, residual, cot, gain, output_cols, kept, tables, weights):
    rows, width = grad.shape
    features = weights[0].shape[0]
    vmem = pl.BlockSpec(memory_space=pltpu.VMEM)
    return pl.pallas_call(
        back_kernel,
        out_shape=(
            jax.ShapeDtypeStruct((rows, width), F32),
            jax.ShapeDtypeStruct((rows, width), BF16),
            jax.ShapeDtypeStruct((1, width), F32),
            jax.ShapeDtypeStruct((1, width), F32),
            jax.ShapeDtypeStruct((rows, features + 2 * HEAD_SIZE), BF16),
            jax.ShapeDtypeStruct((1, features + 2 * HEAD_SIZE), F32),
            jax.ShapeDtypeStruct((rows, width), F32),
            jax.ShapeDtypeStruct((rows, width), BF16),
        ),
        in_specs=[vmem] * 18,
        out_specs=(vmem,) * 8,
        scratch_shapes=[
            pltpu.VMEM((rows, features), BF16),
            pltpu.VMEM((rows, HEAD_SIZE), F32),
            pltpu.VMEM((rows, HEAD_SIZE), F32),
        ],
        compiler_params=pltpu.CompilerParams(vmem_limit_bytes=48 * 1024 * 1024),
        cost_estimate=pl.CostEstimate(
            flops=40 * rows * features * (width + 2 * rows), bytes_accessed=80 * rows * width, transcendentals=0
        ),
    )(tokens, grad, came, residual, cot, gain, output_cols, *kept, *tables, *weights)


def mask_and_tables(lengths, rows):
    ends = jnp.cumsum(lengths)
    starts = ends - lengths
    row = jnp.arange(rows, dtype=jnp.int32)
    inside = (row[:, None] >= starts[None, :]) & (row[:, None] < ends[None, :])
    first = jnp.sum(jnp.where(inside, starts[None, :], 0), axis=1)
    cosine, sine = rotary_tables(row - first, HEAD_SIZE)
    half = HEAD_SIZE // 2
    sine = jnp.concatenate([-sine[:, :half], sine[:, half:]], axis=1)
    return cosine, sine, first[:, None]


def local(
    n_rep,
    tokens,
    query_weight,
    key_weight,
    value_weight,
    query_bias,
    key_bias,
    value_bias,
    output_matrix,
    gate_weight,
    up_weight,
    down_weight,
    attn_gain,
    mlp_gain,
    cotangent,
    seq_lengths,
):
    g = lax.axis_index("grp")
    rows = tokens.shape[0]

    gains = jnp.stack([attn_gain, mlp_gain])
    gains_other = swap(gains)
    lengths_other = swap(seq_lengths)
    cut = output_matrix.shape[1] // 2
    given = jnp.concatenate([half_of(output_matrix, 1 - g, 1), half_of(down_weight, 1 - g, 1)], axis=1)
    shared, came = swap_shared(given, n_rep)
    tokens_other = swap(after(tokens, came))
    gains = in_order(gains, gains_other, g, 1).astype(F32)
    attn_gain_all, mlp_gain_all = gains[0:1], gains[1:2]
    output_cols = in_order(half_of(output_matrix, g, 1), shared[:, :cut], g)
    down_rows = in_order(half_of(down_weight, g, 1), shared[:, cut:], g).T

    weights = (query_weight, key_weight, value_weight)
    biases = tuple(b.astype(F32)[None, :] for b in (query_bias, key_bias, value_bias))

    def begin(token_rows, lengths):
        tables = mask_and_tables(lengths[0], rows)
        normed, queries, keys, values, mixed, logs = front(token_rows, attn_gain_all, weights, biases, tables)
        inputs = token_rows.astype(F32)
        return dict(
            tokens=token_rows,
            unit=inputs * rms_scale(inputs),
            scale=rms_scale(inputs),
            normed=normed,
            kept=(mixed, queries, keys, values, logs),
            tables=tables,
        )

    own = begin(tokens, seq_lengths)
    cotangent_other = swap(after(cotangent, own["kept"][0]))
    own["part"], part_own_b = project(own["kept"][0], output_cols)
    came_other = swap(part_own_b)
    oth = begin(after(tokens_other, own["kept"][0]), after(lengths_other, own["kept"][0]))
    oth["part"], part_oth_b = project(oth["kept"][0], output_cols)
    came_own = swap(after(part_oth_b, part_own_b))

    def middle(kept, came, cot, part_type):
        residual, normed, *wide, grad, grad_b, part = ffn(
            kept["tokens"], kept["part"], came, mlp_gain_all, cot, gate_weight, up_weight, down_rows, part_type
        )
        return dict(residual=residual, normed=normed, wide=wide, grad=grad, grad_b=grad_b, part=part)

    mid_oth = middle(oth, came_other, cotangent_other, BF16)
    grad_came_own = swap(mid_oth["grad_b"])
    mid_own = middle(own, came_own, cotangent, F32)
    grad_came_oth = swap(after(mid_own["grad_b"], grad_came_own))
    down_came = swap(after(mid_oth["part"], grad_came_oth))
    block_out = mid_own["residual"] + mid_own["part"] + down_came.astype(F32)

    def end(mid, came, cot, kept):
        return back(
            kept["tokens"], mid["grad"], came, mid["residual"], cot, mlp_gain_all, output_cols, kept["kept"], kept["tables"], weights
        )

    residual_grad_own, residual_grad_own_b, gain_grad_own, front_gain_own, joined_own, sums_own, front_own, _ = end(
        mid_own, grad_came_own, cotangent, own
    )
    _, residual_grad_oth_b, gain_grad_oth, front_gain_oth, joined_oth, sums_oth, _, front_oth_b = end(
        mid_oth, grad_came_oth, cotangent_other, oth
    )
    mlp_gain_grad = (gain_grad_own + gain_grad_oth)[0]
    front_came = swap(front_oth_b)
    output_grad = mm_tn(
        jnp.concatenate([own["kept"][0], oth["kept"][0]]), jnp.concatenate([residual_grad_own_b, residual_grad_oth_b])
    ).astype(BF16)
    projections = mm_tn(
        jnp.concatenate([joined_own, joined_oth]), jnp.concatenate([own["normed"], oth["normed"]])
    ).astype(BF16)
    attn_gain_grad = (front_gain_own + front_gain_oth)[0]
    front_own = front_own + front_came.astype(F32)
    unit_grad = front_own * attn_gain_all
    input_grad = residual_grad_own + own["scale"] * (
        unit_grad - own["unit"] * jnp.mean(unit_grad * own["unit"], axis=-1, keepdims=True)
    )

    small = jnp.concatenate([(sums_own + sums_oth)[0], half_of(mlp_gain_grad, g, 0), attn_gain_grad])
    count = small.shape[0]
    lines = -(-count // (8 * 128)) * 8
    small = jnp.pad(small, (0, lines * 128 - count)).reshape(lines, 128)
    units, features = gate_weight.shape[0], query_weight.shape[0]
    pieces, small = sum_pool(
        [
            ([mid_oth["wide"][0], mid_own["wide"][0]], [units], True, (0, 1)),
            ([mid_oth["wide"][1], mid_own["wide"][1]], [units], False, (2, 3)),
            ([mid_oth["wide"][2], mid_own["wide"][2]], [units], False, (2, 3)),
            ([output_grad], [features], True, None),
            ([projections], [w.shape[0] for w in weights], False, None),
        ],
        [cotangent_other, cotangent, mid_oth["normed"], mid_own["normed"]],
        small,
        n_rep,
    )
    small = small.reshape(2, -1)
    vectors, at = [], 0
    for piece in (query_bias, key_bias, value_bias, mlp_gain):
        vectors.append(small[0, at : at + piece.shape[0]])
        at += piece.shape[0]
    vectors.append(half_of(small[0, at:count] + small[1, at:count], g, 0))
    half = output_grad.shape[1] // 2

    def owned(piece, count):
        return jnp.concatenate([piece[:half, :count], piece[half:, :count]], axis=1).astype(F32)

    return (
        block_out,
        input_grad,
        pieces[4].astype(F32),
        pieces[5].astype(F32),
        pieces[6].astype(F32),
        vectors[0],
        vectors[1],
        vectors[2],
        owned(pieces[3], features),
        pieces[1].astype(F32),
        pieces[2].astype(F32),
        owned(pieces[0], units),
        vectors[4],
        vectors[3],
    )


def solution(mesh):
    n_rep = mesh.shape["rep"]
    assert mesh.shape["grp"] == 2 and n_rep & (n_rep - 1) == 0
    rows = P(("rep", "grp"), None)
    wide, flat = P("grp", None), P("grp")

    def body(*args):
        return local(n_rep, *args)

    return jax.shard_map(
        body,
        mesh=mesh,
        in_specs=(rows, wide, wide, wide, flat, flat, flat, wide, wide, wide, wide, flat, flat, rows, rows),
        out_specs=(rows, rows, wide, wide, wide, flat, flat, flat, wide, wide, wide, wide, flat, flat),
        check_vma=False,
    )
```

```python
import functools
import math

import jax
import jax.numpy as jnp
from jax import lax
from jax.experimental import pallas as pl
from jax.experimental.pallas import tpu as pltpu
from jax.sharding import PartitionSpec as P


HEAD_SIZE = 128

EPSILON = 1e-06
THETA = 1000000.0

BF16 = jnp.bfloat16
F32 = jnp.float32
MESH = pl.DeviceIdType.MESH


def mm_nt(left, right):
    return lax.dot_general(left, right, (((1,), (1,)), ((), ())), preferred_element_type=F32)


def mm_nn(left, right):
    return lax.dot_general(left, right, (((1,), (0,)), ((), ())), preferred_element_type=F32)


def mm_tn(left, right):
    return lax.dot_general(left, right, (((0,), (0,)), ((), ())), preferred_element_type=F32)


def rotary_tables(position, head_dim):
    half_dim = head_dim // 2
    exponent = jnp.arange(half_dim, dtype=F32) * (2.0 / head_dim)
    frequency = jnp.exp(-exponent * math.log(THETA))
    angles = position.astype(F32)[:, None] * frequency[None, :]
    cosine = jnp.cos(angles)
    sine = jnp.sin(angles)
    return (jnp.concatenate([cosine, cosine], axis=-1), jnp.concatenate([sine, sine], axis=-1))


def rms_scale(values):
    return lax.rsqrt(jnp.mean(values * values, axis=-1, keepdims=True) + EPSILON)


def swap(x):
    return lax.ppermute(x, "grp", [(0, 1), (1, 0)])


def after(x, earlier):
    return lax.optimization_barrier((x, earlier))[0]


def swap_shared(x, n_rep, levels=2):
    levels = min(levels, n_rep.bit_length() - 1)
    me = lax.axis_index("rep")
    count = x.shape[0] >> levels
    came = piece = swap(lax.dynamic_slice_in_dim(x, (me & ((1 << levels) - 1)) * count, count, 0))
    for b in range(levels):
        shared = lax.ppermute(came, "rep", [(i, i ^ (1 << b)) for i in range(n_rep)])
        came = in_order(came, shared, (me >> b) & 1)
    return came, piece


def in_order(mine, other, g, axis=0):
    first = jnp.where(g == 0, mine, other)
    second = jnp.where(g == 0, other, mine)
    return jnp.concatenate([first, second], axis)


def half_of(x, which, axis):
    size = x.shape[axis] // 2
    return lax.dynamic_slice_in_dim(x, which * size, size, axis)


def rows_loop(count, step, body):
    def one(i, carry):
        body(pl.multiple_of(i * step, step), step)
        return carry

    lax.fori_loop(0, count // step, one, 0)


def pool_kernel(plan, groups, n_factors, slots, n_rep, *refs):
    n_parts = sum(2 if made else len(parts) for _, parts, _, _, _, made in groups)
    n_outs = sum(1 if cross else len(cuts) for _, _, _, cuts, cross, _ in groups)
    ins, factors, refs = refs[:n_parts], refs[n_parts : n_parts + n_factors], refs[n_parts + n_factors :]
    small_ref, refs = refs[0], refs[1:]
    outs, small_out, refs = refs[:n_outs], refs[n_outs], refs[n_outs + 1 :]
    pool, full, inbox, flipped, lefts, small_box, in_sem, left_sem, out_sem, *refs = refs
    send_sem, recv_sem, small_send, small_recv = refs
    me, g = lax.axis_index("rep"), lax.axis_index("grp")
    bits = n_rep.bit_length() - 1
    half = pool.shape[1] // 2

    barrier = pltpu.get_barrier_semaphore()
    for b in range(bits):
        pl.semaphore_signal(barrier, inc=1, device_id={"rep": me ^ (1 << b)}, device_id_type=MESH)
    pl.semaphore_signal(barrier, inc=1, device_id={"grp": 1 - g}, device_id_type=MESH)

    loads, at = [], 0
    makers = {}
    for k, (base, parts, end, _, _, made) in enumerate(groups):
        loads.append([])
        if made:
            makers[k] = ins[at : at + 2], [factors[f] for f in made]
            at, base = at + 2, base + parts[0]
        else:
            for count in parts:
                loads[-1].append(pltpu.make_async_copy(ins[at], pool.at[pl.ds(base, count)], in_sem.at[at]))
                loads[-1][-1].start()
                base, at = base + count, at + 1
        if base < end:
            pool[pl.ds(base, end - base), :] = jnp.zeros((end - base, pool.shape[1]), BF16)
    made_units = [u for u, unit in enumerate(plan) if unit[3] in makers]
    fetched = {}

    def fetch(k):
        if k < len(made_units):
            u = made_units[k]
            start, size, _, group, _ = plan[u]
            base, parts = groups[group][:2]
            count = min(size, base + parts[0] - start)
            fetched[u] = count, []
            for side, source in enumerate(makers[group][0]):
                copy = pltpu.make_async_copy(
                    source.at[pl.ds(start - base, count)], lefts.at[k % slots, side, pl.ds(0, count)], left_sem.at[k, side]
                )
                copy.start()
                fetched[u][1].append(copy)

    def make(u):
        k = made_units.index(u)
        start, _, _, group, _ = plan[u]
        count, waits = fetched[u]
        for copy in waits:
            copy.wait()
        first, second = makers[group][1]

        def one(i, step):
            rows = pl.ds(pl.multiple_of(i, 16), step)
            product = mm_nn(lefts[k % slots, 0, rows, :], first[...]) + mm_nn(lefts[k % slots, 1, rows, :], second[...])
            pool[pl.ds(pl.multiple_of(start + i, 16), step), :] = product.astype(BF16)

        rows_loop(count, count // 2 if count % 32 == 0 else count, one)
        fetch(k + slots)

    for k in range(slots):
        fetch(k)
    small_box[0] = small_ref[...]
    pl.semaphore_wait(barrier, bits + 1)

    copies, state, box_at, used = {}, {}, {}, 0
    for u, (start, size, order, group, cross) in enumerate(plan):
        n = size
        for s in range(bits):
            n //= 2
            box_at[u, s] = used
            used += n
    loaded, numbers, leaving, flips, count_of_flips = set(), {}, [], [], [0]

    def remote(source, target, key, there):
        at = numbers.setdefault(key, len(numbers))
        copies[key] = pltpu.make_async_remote_copy(
            src_ref=source,
            dst_ref=target,
            send_sem=send_sem.at[at],
            recv_sem=recv_sem.at[at],
            device_id=there,
            device_id_type=MESH,
        )
        copies[key].start()

    def bit_of(b):
        return (me >> b) & 1

    def advance(u, step):
        start, size, order, group, cross = plan[u]
        kinds = ["halve"] * bits + ["cross"] * cross + ["double"] * bits + ["out"]
        if step == 0:
            if group not in loaded:
                loaded.add(group)
                for load in loads[group]:
                    load.wait()
            if group in makers:
                make(u)
            state[u] = [jnp.int32(start), size]
        else:
            copies[u, step - 1].wait()
            before = kinds[step - 1]
            off, n = state[u]
            if before == "halve":
                n //= 2
                at = box_at[u, step - 1]
                keep = pl.multiple_of(off + bit_of(order[step - 1]) * n, n)
                target = full if kinds[step] == "double" else pool

                def add(i, count):
                    there = pl.ds(pl.multiple_of(keep + i, 16), count)
                    here = pl.ds(pl.multiple_of(at + i, 16), count)
                    target[there, :] = (pool[there, :].astype(F32) + inbox[here, :].astype(F32)).astype(BF16)

                rows_loop(n, 16 if n % 32 else 32, add)
                state[u] = [keep, n]
            elif before == "double":
                b = order[2 * bits + cross - step]
                state[u] = [pl.multiple_of(off - bit_of(b) * n, n), 2 * n]
        off, n = state[u]
        kind = kinds[step]
        if kind == "halve":
            n //= 2
            b = order[step]
            give = pl.multiple_of(off + (1 - bit_of(b)) * n, n)
            target = inbox.at[pl.ds(box_at[u, step], n)]
            remote(pool.at[pl.ds(give, n)], target, (u, step), {"rep": me ^ (1 << b)})
        elif kind == "cross":
            rows = pl.ds(off, n)
            mine = pl.ds(pl.multiple_of(g * half, 128), half)
            theirs = pl.ds(pl.multiple_of((1 - g) * half, 128), half)
            remote(pool.at[rows, theirs], full.at[rows, mine], (u, step), {"grp": 1 - g})
            full[rows, mine] = pool[rows, mine]
        elif kind == "double":
            b = order[2 * bits + cross - 1 - step]
            block = pl.ds(off, n)
            remote(full.at[block], full.at[block], (u, step), {"rep": me ^ (1 << b)})
        else:
            first = sum(1 if c else len(cuts) for _, _, _, cuts, c, _ in groups[:group])
            base, cuts = groups[group][0], groups[group][3]
            wanted = []
            if cross:
                slot = count_of_flips[0] % slots
                if count_of_flips[0] >= slots:
                    flips[count_of_flips[0] - slots].wait()
                count_of_flips[0] += 1

                def flip(i, count):
                    piece = full[pl.ds(pl.multiple_of(start + i, 128), count), :].astype(F32)
                    flipped[slot, :, pl.ds(pl.multiple_of(i, 128), count)] = piece.T.astype(BF16)

                rows_loop(size, 128, flip)
                wanted.append((flipped.at[slot, :, pl.ds(0, size)], outs[first].at[:, pl.ds(start - base, size)]))
            for k, count in enumerate(() if cross else cuts):
                low, high = max(base, start), min(base + count, start + size)
                if low < high:
                    wanted.append((full.at[pl.ds(low, high - low)], outs[first + k].at[pl.ds(low - base, high - low)]))
                base += count
            for source, target in wanted:
                copy = pltpu.make_async_copy(source, target, out_sem.at[len(leaving) + len(flips)])
                copy.start()
                (flips if cross else leaving).append(copy)

    def advance_small(s):
        if s > 0:
            copies["small", s - 1].wait()
            if s <= bits:
                small_box[2 * s] = small_box[2 * s - 2] + small_box[2 * s - 1]
        if s <= bits:
            copies["small", s] = pltpu.make_async_remote_copy(
                src_ref=small_box.at[2 * s],
                dst_ref=small_box.at[2 * s + 1],
                send_sem=small_send.at[s],
                recv_sem=small_recv.at[s],
                device_id={"rep": me ^ (1 << s)} if s < bits else {"grp": 1 - g},
                device_id_type=MESH,
            )
            copies["small", s].start()
        else:
            small_out[0] = small_box[2 * bits]
            small_out[1] = small_box[2 * bits + 1]

    steps = [2 * bits + 1 + cross for *_, cross in plan]
    for t in range(max(u + n for u, n in enumerate(steps))):
        for u in range(len(plan)):
            if 0 <= t - u < steps[u]:
                advance(u, t - u)
        if t <= bits + 1:
            advance_small(t)
    for copy in leaving + flips[-slots:]:
        copy.wait()


def sum_pool(groups, factors, small, n_rep):
    bits = n_rep.bit_length() - 1
    straight = tuple(range(bits))
    grain = 16 * n_rep
    unit = max(768 // grain, 1) * grain
    flat = [a for arrays, *_ in groups for a in arrays]
    width = factors[0].shape[1]
    slots = 2 if n_rep <= 16 else 1
    plan, places, outs, base = [], [], [], 0
    for k, (arrays, cuts, cross, made) in enumerate(groups):
        counts = [a.shape[0] for a in arrays[: 1 if made else None]]
        end = base + -(-sum(counts) // grain) * grain
        places.append((base, counts, end, cuts, cross, made))
        for start in range(base, end, unit):
            plan.append((start, min(unit, end - start), straight, k, int(cross)))
        outs += [(width, end - base)] if cross else [(count, width) for count in cuts]
        base = end
    box = sum(size - size // n_rep for _, size, *_ in plan)
    n_copies = sum(2 * bits + cross for *_, cross in plan)
    any_space = pl.BlockSpec(memory_space=pl.ANY)
    vmem = pl.BlockSpec(memory_space=pltpu.VMEM)
    *pieces, sums = pl.pallas_call(
        functools.partial(pool_kernel, plan, places, len(factors), slots, n_rep),
        out_shape=tuple(jax.ShapeDtypeStruct(shape, BF16) for shape in outs)
        + (jax.ShapeDtypeStruct((2,) + small.shape, F32),),
        in_specs=[any_space] * len(flat) + [vmem] * (len(factors) + 1),
        out_specs=(any_space,) * len(outs) + (vmem,),
        scratch_shapes=[
            pltpu.VMEM((base, width), BF16),
            pltpu.VMEM((base, width), BF16),
            pltpu.VMEM((box, width), BF16),
            pltpu.VMEM((slots, width, unit), BF16),
            pltpu.VMEM((slots, 2, unit, factors[0].shape[0]), BF16),
            pltpu.VMEM((2 * bits + 2,) + small.shape, F32),
            pltpu.SemaphoreType.DMA((len(flat),)),
            pltpu.SemaphoreType.DMA((len(plan), 2)),
            pltpu.SemaphoreType.DMA((len(plan) + len(outs),)),
            pltpu.SemaphoreType.DMA((n_copies,)),
            pltpu.SemaphoreType.DMA((n_copies,)),
            pltpu.SemaphoreType.DMA((bits + 1,)),
            pltpu.SemaphoreType.DMA((bits + 1,)),
        ],
        compiler_params=pltpu.CompilerParams(
            collective_id=0, has_side_effects=True, vmem_limit_bytes=62 * 1024 * 1024
        ),
    )(*flat, *factors, small)
    return pieces, sums


def ffn_kernel(
    tokens, part, came, gain, cot, gate, up, down, residual, n2, hid_out, gg_out, ug_out, ng_out, ngb_out, dp_out, ng_acc, dp_acc
):
    step = pl.program_id(0)

    @pl.when(step == 0)
    def _():
        total = tokens[...].astype(F32) + part[...] + came[...].astype(F32)
        residual[...] = total
        n2[...] = (total * rms_scale(total) * gain[...]).astype(BF16)
        ng_acc[...] = jnp.zeros_like(ng_acc)
        dp_acc[...] = jnp.zeros_like(dp_acc)

    gate_pre = mm_nt(gate[...], n2[...])
    up_proj = mm_nt(up[...], n2[...])
    hidden_grad = mm_nt(down[...], cot[...])
    sigmoid = 1.0 / (1.0 + jnp.exp(-gate_pre))
    activated = gate_pre * sigmoid
    hidden = (activated * up_proj).astype(BF16)
    gate_grad = (hidden_grad * up_proj * sigmoid * (1.0 + gate_pre * (1.0 - sigmoid))).astype(BF16)
    up_grad = (hidden_grad * activated).astype(BF16)
    hid_out[...] = hidden
    gg_out[...] = gate_grad
    ug_out[...] = up_grad
    ng_acc[...] += mm_tn(gate_grad, gate[...]) + mm_tn(up_grad, up[...])
    dp_acc[...] += mm_tn(hidden, down[...])

    @pl.when(step == pl.num_programs(0) - 1)
    def _():
        ng_out[...] = ng_acc[...]
        ngb_out[...] = ng_acc[...].astype(BF16)
        dp_out[...] = dp_acc[...].astype(dp_out.dtype)


def block_of(count, limit, grain):
    return max(d for d in range(grain, limit + 1, grain) if count % d == 0)


def ffn(tokens, part, came, gain, cot, gate, up, down, part_type):
    rows, width = tokens.shape
    units = gate.shape[0]
    block = block_of(units, 512, 16)
    whole = pl.BlockSpec((rows, width), lambda i: (0, 0))
    cut = pl.BlockSpec((block, width), lambda i: (i, 0))
    cut_rows = pl.BlockSpec((block, rows), lambda i: (i, 0))
    wide = jax.ShapeDtypeStruct((units, rows), BF16)
    return pl.pallas_call(
        ffn_kernel,
        grid=(units // block,),
        out_shape=(
            jax.ShapeDtypeStruct((rows, width), F32),
            jax.ShapeDtypeStruct((rows, width), BF16),
            wide,
            wide,
            wide,
            jax.ShapeDtypeStruct((rows, width), F32),
            jax.ShapeDtypeStruct((rows, width), BF16),
            jax.ShapeDtypeStruct((rows, width), part_type),
        ),
        in_specs=[whole, whole, whole, pl.BlockSpec((1, width), lambda i: (0, 0)), whole, cut, cut, cut],
        out_specs=(whole, whole, cut_rows, cut_rows, cut_rows, whole, whole, whole),
        scratch_shapes=[pltpu.VMEM((rows, width), F32), pltpu.VMEM((rows, width), F32)],
        compiler_params=pltpu.CompilerParams(vmem_limit_bytes=56 * 1024 * 1024),
        cost_estimate=pl.CostEstimate(
            flops=12 * units * rows * width, bytes_accessed=12 * units * width, transcendentals=units * rows
        ),
    )(tokens, part, came, gain, cot, gate, up, down)


def turn(x):
    return pltpu.roll(x, HEAD_SIZE // 2, 1)


def head_at(h):
    return pl.ds(pl.multiple_of(h * HEAD_SIZE, HEAD_SIZE), HEAD_SIZE)


def masked_scores(query, key, first, row, count, limit):
    scores = mm_nt(query, key) * (1.0 / math.sqrt(HEAD_SIZE))
    at = lax.broadcasted_iota(jnp.int32, (count, limit), 1)
    line = lax.broadcasted_iota(jnp.int32, (count, limit), 0) + row
    return jnp.where((at <= line) & (at >= first), scores, -1e30)


def front_kernel(
    tokens, gain, qw, kw, vw, qb, kb, vb, cos, sin, first, normed, queries, keys, values, mixed, logs
):
    rows = tokens.shape[0]
    heads = qw.shape[0] // HEAD_SIZE
    block = math.gcd(rows, 256)
    inputs = tokens[...].astype(F32)
    normed[...] = (inputs * rms_scale(inputs) * gain[...]).astype(BF16)
    keys_pre = mm_nt(normed[...], kw[...]) + kb[...]
    keys[...] = (keys_pre * cos[...] + turn(keys_pre) * sin[...]).astype(BF16)
    values[...] = (mm_nt(normed[...], vw[...]) + vb[...]).astype(BF16)
    logs[...] = jnp.zeros_like(logs)
    lane = lax.broadcasted_iota(jnp.int32, (block, HEAD_SIZE), 1)

    def one_head(h, carry):
        lanes = head_at(h)
        pre = mm_nt(normed[...], qw[lanes, :]) + qb[:, lanes]
        queries[:, lanes] = (pre * cos[...] + turn(pre) * sin[...]).astype(BF16)
        for row in range(0, rows, block):
            here, limit = pl.ds(row, block), row + block
            scores = masked_scores(queries[here, lanes], keys[:limit, :], first[here, :], row, block, limit)
            peak = jnp.max(scores, axis=1, keepdims=True)
            weights = jnp.exp(scores - peak)
            sums = jnp.sum(weights, axis=1, keepdims=True)
            logs[here, :] = jnp.where(lane == h, peak + jnp.log(sums), logs[here, :])
            probs = (weights * (1.0 / sums)).astype(BF16)
            mixed[here, lanes] = mm_nn(probs, values[:limit, :]).astype(BF16)
        return carry

    lax.fori_loop(0, heads, one_head, 0)


def front(tokens, gain, weights, biases, tables):
    rows, width = tokens.shape
    features = weights[0].shape[0]
    vmem = pl.BlockSpec(memory_space=pltpu.VMEM)
    return pl.pallas_call(
        front_kernel,
        out_shape=(
            jax.ShapeDtypeStruct((rows, width), BF16),
            jax.ShapeDtypeStruct((rows, features), BF16),
            jax.ShapeDtypeStruct((rows, HEAD_SIZE), BF16),
            jax.ShapeDtypeStruct((rows, HEAD_SIZE), BF16),
            jax.ShapeDtypeStruct((rows, features), BF16),
            jax.ShapeDtypeStruct((rows, HEAD_SIZE), F32),
        ),
        in_specs=[vmem] * 11,
        out_specs=(vmem,) * 6,
        compiler_params=pltpu.CompilerParams(vmem_limit_bytes=48 * 1024 * 1024),
        cost_estimate=pl.CostEstimate(
            flops=40 * rows * features * (width + rows), bytes_accessed=80 * rows * width, transcendentals=0
        ),
    )(tokens, gain, *weights, *biases, *tables)


def project_kernel(mixed, ow, part, part_b):
    part[...] = mm_nt(mixed[...], ow[...])
    part_b[...] = part[...].astype(BF16)


def project(mixed, output_cols):
    shape = mixed.shape[0], output_cols.shape[0]
    vmem = pl.BlockSpec(memory_space=pltpu.VMEM)
    return pl.pallas_call(
        project_kernel,
        out_shape=(jax.ShapeDtypeStruct(shape, F32), jax.ShapeDtypeStruct(shape, BF16)),
        in_specs=[vmem] * 2,
        out_specs=(vmem,) * 2,
        compiler_params=pltpu.CompilerParams(vmem_limit_bytes=16 * 1024 * 1024),
        cost_estimate=pl.CostEstimate(
            flops=2 * mixed.size * shape[1], bytes_accessed=16 * mixed.size, transcendentals=0
        ),
    )(mixed, output_cols)


def back_kernel(
    tokens, grad, came, residual, cot, gain, ow, mixed, queries, keys, values, logs, cos, sin, first, qw, kw, vw,
    residual_grad, residual_grad_b, gain_grad, front_gain_grad, joined, sums, out, out_b, mg, dk, dv
):
    rows, features = queries.shape
    heads = features // HEAD_SIZE
    block = math.gcd(rows, 256)
    scale = 1.0 / math.sqrt(HEAD_SIZE)
    normed_grad = grad[...] + came[...].astype(F32)
    norm = rms_scale(residual[...])
    unit = residual[...] * norm
    gain_grad[...] = jnp.sum(normed_grad * unit, axis=0, keepdims=True)
    unit_grad = normed_grad * gain[...]
    along = jnp.mean(unit_grad * unit, axis=1, keepdims=True)
    residual_grad[...] = cot[...].astype(F32) + norm * (unit_grad - unit * along)
    residual_grad_b[...] = residual_grad[...].astype(BF16)
    mg[...] = mm_nn(residual_grad_b[...], ow[...]).astype(BF16)
    dk[...] = jnp.zeros_like(dk)
    dv[...] = jnp.zeros_like(dv)
    lane = lax.broadcasted_iota(jnp.int32, (block, HEAD_SIZE), 1)

    def one_head(h, carry):
        lanes = head_at(h)
        total = jnp.zeros((1, HEAD_SIZE), F32)
        for row in range(0, rows, block):
            here, limit = pl.ds(row, block), row + block
            query, grads = queries[here, lanes], mg[here, lanes]
            scores = masked_scores(query, keys[:limit, :], first[here, :], row, block, limit)
            log_total = jnp.sum(jnp.where(lane == h, logs[here, :], 0.0), axis=1, keepdims=True)
            probs = jnp.exp(scores - log_total)
            delta = jnp.sum(grads.astype(F32) * mixed[here, lanes].astype(F32), axis=1, keepdims=True)
            probs_grad = mm_nt(grads, values[:limit, :])
            score_grad = (probs * (probs_grad - delta) * scale).astype(BF16)
            dv[:limit, :] += mm_tn(probs.astype(BF16), grads)
            dk[:limit, :] += mm_tn(score_grad, query)
            dq = mm_nn(score_grad, keys[:limit, :])
            dq = dq * cos[here, :] - turn(dq) * sin[here, :]
            total = total + jnp.sum(dq, axis=0, keepdims=True)
            joined[here, lanes] = dq.astype(BF16)
        sums[:, lanes] = total
        return carry

    lax.fori_loop(0, heads, one_head, 0)
    keys_grad = dk[...] * cos[...] - turn(dk[...]) * sin[...]
    for k, piece in enumerate((keys_grad, dv[...])):
        lanes = pl.ds(features + k * HEAD_SIZE, HEAD_SIZE)
        sums[:, lanes] = jnp.sum(piece, axis=0, keepdims=True)
        joined[:, lanes] = piece.astype(BF16)
    out[...] = (
        mm_nn(joined[:, :features], qw[...])
        + mm_nn(joined[:, features : features + HEAD_SIZE], kw[...])
        + mm_nn(joined[:, features + HEAD_SIZE :], vw[...])
    )
    out_b[...] = out[...].astype(BF16)
    inputs = tokens[...].astype(F32)
    front_gain_grad[...] = jnp.sum(out[...] * (inputs * rms_scale(inputs)), axis=0, keepdims=True)


def back(tokens, grad, came, residual, cot, gain, output_cols, kept, tables, weights):
    rows, width = grad.shape
    features = weights[0].shape[0]
    vmem = pl.BlockSpec(memory_space=pltpu.VMEM)
    return pl.pallas_call(
        back_kernel,
        out_shape=(
            jax.ShapeDtypeStruct((rows, width), F32),
            jax.ShapeDtypeStruct((rows, width), BF16),
            jax.ShapeDtypeStruct((1, width), F32),
            jax.ShapeDtypeStruct((1, width), F32),
            jax.ShapeDtypeStruct((rows, features + 2 * HEAD_SIZE), BF16),
            jax.ShapeDtypeStruct((1, features + 2 * HEAD_SIZE), F32),
            jax.ShapeDtypeStruct((rows, width), F32),
            jax.ShapeDtypeStruct((rows, width), BF16),
        ),
        in_specs=[vmem] * 18,
        out_specs=(vmem,) * 8,
        scratch_shapes=[
            pltpu.VMEM((rows, features), BF16),
            pltpu.VMEM((rows, HEAD_SIZE), F32),
            pltpu.VMEM((rows, HEAD_SIZE), F32),
        ],
        compiler_params=pltpu.CompilerParams(vmem_limit_bytes=48 * 1024 * 1024),
        cost_estimate=pl.CostEstimate(
            flops=40 * rows * features * (width + 2 * rows), bytes_accessed=80 * rows * width, transcendentals=0
        ),
    )(tokens, grad, came, residual, cot, gain, output_cols, *kept, *tables, *weights)


def mask_and_tables(lengths, rows):
    ends = jnp.cumsum(lengths)
    starts = ends - lengths
    row = jnp.arange(rows, dtype=jnp.int32)
    inside = (row[:, None] >= starts[None, :]) & (row[:, None] < ends[None, :])
    first = jnp.sum(jnp.where(inside, starts[None, :], 0), axis=1)
    cosine, sine = rotary_tables(row - first, HEAD_SIZE)
    half = HEAD_SIZE // 2
    sine = jnp.concatenate([-sine[:, :half], sine[:, half:]], axis=1)
    return cosine, sine, first[:, None]


def local(
    n_rep,
    tokens,
    query_weight,
    key_weight,
    value_weight,
    query_bias,
    key_bias,
    value_bias,
    output_matrix,
    gate_weight,
    up_weight,
    down_weight,
    attn_gain,
    mlp_gain,
    cotangent,
    seq_lengths,
):
    g = lax.axis_index("grp")
    rows = tokens.shape[0]

    gains = jnp.stack([attn_gain, mlp_gain])
    gains_other = swap(gains)
    lengths_other = swap(seq_lengths)
    cut = output_matrix.shape[1] // 2
    given = jnp.concatenate([half_of(output_matrix, 1 - g, 1), half_of(down_weight, 1 - g, 1)], axis=1)
    shared, came = swap_shared(given, n_rep)
    tokens_other = swap(after(tokens, came))
    gains = in_order(gains, gains_other, g, 1).astype(F32)
    attn_gain_all, mlp_gain_all = gains[0:1], gains[1:2]
    output_cols = in_order(half_of(output_matrix, g, 1), shared[:, :cut], g)
    down_rows = in_order(half_of(down_weight, g, 1), shared[:, cut:], g).T

    weights = (query_weight, key_weight, value_weight)
    biases = tuple(b.astype(F32)[None, :] for b in (query_bias, key_bias, value_bias))

    def begin(token_rows, lengths):
        tables = mask_and_tables(lengths[0], rows)
        normed, queries, keys, values, mixed, logs = front(token_rows, attn_gain_all, weights, biases, tables)
        inputs = token_rows.astype(F32)
        return dict(
            tokens=token_rows,
            unit=inputs * rms_scale(inputs),
            scale=rms_scale(inputs),
            normed=normed,
            kept=(mixed, queries, keys, values, logs),
            tables=tables,
        )

    own = begin(tokens, seq_lengths)
    cotangent_other = swap(after(cotangent, own["kept"][0]))
    own["part"], part_own_b = project(own["kept"][0], output_cols)
    came_other = swap(part_own_b)
    oth = begin(after(tokens_other, own["kept"][0]), after(lengths_other, own["kept"][0]))
    oth["part"], part_oth_b = project(oth["kept"][0], output_cols)
    came_own = swap(after(part_oth_b, came_other))

    def middle(kept, came, cot, part_type):
        residual, normed, *wide, grad, grad_b, part = ffn(
            kept["tokens"], kept["part"], came, mlp_gain_all, cot, gate_weight, up_weight, down_rows, part_type
        )
        return dict(residual=residual, normed=normed, wide=wide, grad=grad, grad_b=grad_b, part=part)

    mid_oth = middle(oth, came_other, cotangent_other, BF16)
    grad_came_own = swap(mid_oth["grad_b"])
    mid_own = middle(own, came_own, cotangent, F32)
    grad_came_oth = swap(after(mid_own["grad_b"], grad_came_own))
    down_came = swap(after(mid_oth["part"], grad_came_oth))
    block_out = mid_own["residual"] + mid_own["part"] + down_came.astype(F32)

    def end(mid, came, cot, kept):
        return back(
            kept["tokens"], mid["grad"], came, mid["residual"], cot, mlp_gain_all, output_cols, kept["kept"], kept["tables"], weights
        )

    residual_grad_own, residual_grad_own_b, gain_grad_own, front_gain_own, joined_own, sums_own, front_own, _ = end(
        mid_own, grad_came_own, cotangent, own
    )
    _, residual_grad_oth_b, gain_grad_oth, front_gain_oth, joined_oth, sums_oth, _, front_oth_b = end(
        mid_oth, grad_came_oth, cotangent_other, oth
    )
    mlp_gain_grad = (gain_grad_own + gain_grad_oth)[0]
    front_came = swap(front_oth_b)
    output_grad = mm_tn(
        jnp.concatenate([own["kept"][0], oth["kept"][0]]), jnp.concatenate([residual_grad_own_b, residual_grad_oth_b])
    ).astype(BF16)
    projections = mm_tn(
        jnp.concatenate([joined_own, joined_oth]), jnp.concatenate([own["normed"], oth["normed"]])
    ).astype(BF16)
    attn_gain_grad = (front_gain_own + front_gain_oth)[0]
    front_own = front_own + front_came.astype(F32)
    unit_grad = front_own * attn_gain_all
    input_grad = residual_grad_own + own["scale"] * (
        unit_grad - own["unit"] * jnp.mean(unit_grad * own["unit"], axis=-1, keepdims=True)
    )

    small = jnp.concatenate([(sums_own + sums_oth)[0], half_of(mlp_gain_grad, g, 0), attn_gain_grad])
    count = small.shape[0]
    lines = -(-count // (8 * 128)) * 8
    small = jnp.pad(small, (0, lines * 128 - count)).reshape(lines, 128)
    units, features = gate_weight.shape[0], query_weight.shape[0]
    pieces, small = sum_pool(
        [
            ([mid_oth["wide"][0], mid_own["wide"][0]], [units], True, (0, 1)),
            ([mid_oth["wide"][1], mid_own["wide"][1]], [units], False, (2, 3)),
            ([mid_oth["wide"][2], mid_own["wide"][2]], [units], False, (2, 3)),
            ([output_grad], [features], True, None),
            ([projections], [w.shape[0] for w in weights], False, None),
        ],
        [cotangent_other, cotangent, mid_oth["normed"], mid_own["normed"]],
        small,
        n_rep,
    )
    small = small.reshape(2, -1)
    vectors, at = [], 0
    for piece in (query_bias, key_bias, value_bias, mlp_gain):
        vectors.append(small[0, at : at + piece.shape[0]])
        at += piece.shape[0]
    vectors.append(half_of(small[0, at:count] + small[1, at:count], g, 0))
    half = output_grad.shape[1] // 2

    def owned(piece, count):
        return jnp.concatenate([piece[:half, :count], piece[half:, :count]], axis=1).astype(F32)

    return (
        block_out,
        input_grad,
        pieces[4].astype(F32),
        pieces[5].astype(F32),
        pieces[6].astype(F32),
        vectors[0],
        vectors[1],
        vectors[2],
        owned(pieces[3], features),
        pieces[1].astype(F32),
        pieces[2].astype(F32),
        owned(pieces[0], units),
        vectors[4],
        vectors[3],
    )


def solution(mesh):
    n_rep = mesh.shape["rep"]
    assert mesh.shape["grp"] == 2 and n_rep & (n_rep - 1) == 0
    rows = P(("rep", "grp"), None)
    wide, flat = P("grp", None), P("grp")

    def body(*args):
        return local(n_rep, *args)

    return jax.shard_map(
        body,
        mesh=mesh,
        in_specs=(rows, wide, wide, wide, flat, flat, flat, wide, wide, wide, wide, flat, flat, rows, rows),
        out_specs=(rows, rows, wide, wide, wide, flat, flat, flat, wide, wide, wide, wide, flat, flat),
        check_vma=False,
    )
```
